8 devices in a mesh: data: 1 (over z), outer: 2 (over y), expert: 4 (over x, core).
Axes of the slice: x: 2, y: 2, z: 1, core: 2. Of those that a mesh axis runs over, the one named last changes fastest.
Arguments:
- x: bfloat16 [2048, 2048], P(('data', 'outer', 'expert'))
- wr: bfloat16 [2048, 128], replicated
- idx: int32 [2048, 8], P(('data', 'outer', 'expert'))
- w1: bfloat16 [128, 2048, 768], P(('outer', 'expert'))
- w3: bfloat16 [128, 2048, 768], P(('outer', 'expert'))
- w2: bfloat16 [128, 768, 2048], P(('outer', 'expert'))
Outputs:
- output: bfloat16 [2048, 2048], P(('data', 'outer', 'expert'))
All inputs are finite; a program needn't handle non-finite values.
Results may differ from the reference program's by a relative error of at most 0.00813279.
Values are sent between devices in bfloat16 or wider.
A program may use at most 1 GiB of HBM per device.

```python
import jax
import jax.numpy as jnp
from jax import lax

OUTER = 2
EXPERT = 4
T = 256
D = 2048
FF = 768
E = 128
TOP = 8

N_DEV = OUTER * EXPERT
CAP = 2 * T * TOP // E


def _w(key, shape, scale):
    ks = jax.random.split(key, shape[0])
    return lax.map(lambda kk: (scale * jax.random.normal(kk, shape[1:], jnp.float32)).astype(jnp.bfloat16), ks)


def setup_inputs(seed: int = 0, part: int = 0) -> dict:
    key = jax.random.key(seed)
    kr, k1, k3, k2 = jax.random.split(key, 4)
    kp = jax.random.fold_in(key, part)
    kx, _, _ = jax.random.split(kp, 3)
    kb1, kb2, kb3 = jax.random.split(jax.random.fold_in(kp, 7), 3)
    x = jax.random.normal(kx, (N_DEV * T, D), jnp.float32).astype(jnp.bfloat16)
    wr = (1.5 * D ** -0.5 * jax.random.normal(kr, (D, E), jnp.float32)).astype(jnp.bfloat16)
    w1 = _w(k1, (E, D, FF), D ** -0.5)
    w3 = _w(k3, (E, D, FF), D ** -0.5)
    w2 = _w(k2, (E, FF, D), FF ** -0.5)
    nc = N_DEV * T // E
    rot = jax.random.randint(kb1, (N_DEV,), 0, E, jnp.int32)
    base = jnp.arange(E, dtype=jnp.int32) // 2
    p = jax.vmap(lambda kk: jax.random.permutation(kk, base))(jax.random.split(kb2, nc))
    p = p + jnp.repeat(rot, T // E)[:, None]
    w = min(2 * TOP, E)
    off = jax.vmap(lambda kk: jax.random.permutation(kk, w)[:TOP])(jax.random.split(kb3, nc))
    idx = ((p[:, :, None] + off[:, None, :]) % E).reshape(N_DEV * T, TOP).astype(jnp.int32)
    return {'x': x, 'wr': wr, 'idx': idx, 'w1': w1, 'w3': w3, 'w2': w2}


def _ranks(e, num):
    order = jnp.argsort(e, stable=True)
    se = e[order]
    first = jnp.searchsorted(se, jnp.arange(num, dtype=jnp.int32), side='left').astype(jnp.int32)
    r = jnp.arange(e.shape[0], dtype=jnp.int32) - first[se]
    return jnp.zeros_like(e).at[order].set(r)


def reference(x, wr, idx, w1, w3, w2):
    logits = jnp.dot(x, wr, preferred_element_type=jnp.float32)
    g = jax.nn.softmax(jnp.take_along_axis(logits, idx, axis=1), axis=-1)
    eb = idx.reshape(N_DEV, T * TOP)
    r = jax.vmap(lambda v: _ranks(v, E))(eb).reshape(-1)
    e = eb.reshape(-1)
    src = jnp.arange(N_DEV * T * TOP, dtype=jnp.int32) // (T * TOP)
    tok = jnp.arange(N_DEV * T * TOP, dtype=jnp.int32) // TOP
    pos = jnp.where(r < CAP, e * (N_DEV * CAP) + src * CAP + r, E * N_DEV * CAP)
    tab = jnp.full((E * N_DEV * CAP,), N_DEV * T, jnp.int32).at[pos].set(tok, mode='drop').reshape(E, N_DEV * CAP)
    gt = jnp.zeros((E * N_DEV * CAP,), jnp.float32).at[pos].set(g.reshape(-1), mode='drop').reshape(E, N_DEV * CAP)

    def step(y, inp):
        t, gw, a1, a3, a2 = inp
        xe = jnp.take(x, t, axis=0, mode='fill', fill_value=0)
        a = jnp.dot(xe, a1, preferred_element_type=jnp.float32)
        b = jnp.dot(xe, a3, preferred_element_type=jnp.float32)
        h = (jax.nn.silu(a) * b).astype(jnp.bfloat16)
        o = jnp.dot(h, a2, preferred_element_type=jnp.float32).astype(jnp.bfloat16)
        return y.at[t].add(gw[:, None] * o.astype(jnp.float32), mode='drop'), None

    y, _ = lax.scan(step, jnp.zeros((N_DEV * T, D), jnp.float32), (tab, gt, w1, w3, w2))
    return y.astype(jnp.bfloat16)
```

```python
import functools

import jax
import jax.numpy as jnp
from jax import lax
from jax.experimental import pallas as pl
from jax.experimental.pallas import tpu as pltpu
from jax.sharding import PartitionSpec as P

MESH = pl.DeviceIdType.MESH
BF = jnp.bfloat16
F32 = jnp.float32
U = 256
CW = 128
NWT = 3
NW2 = 4


def _dot(a, b):
    return jnp.dot(a, b, preferred_element_type=F32)


def kernel(x_hbm, wr_hbm, idx_hbm, w1_hbm, w3_hbm, w2_hbm, out_ref,
           X, WR, IDX, ET, EX, POS, HT, W, XIN, ACC, WT, W2T, OB,
           xsem, wtsem, w2sem, dsend, drecv, esend, erecv,
           d2s, d2r, p1s, p1r, p2s, p2r, ready):
    T, D = x_hbm.shape
    E = wr_hbm.shape[1]
    EL, _, FF = w1_hbm.shape
    K = idx_hbm.shape[1]
    C = 2 * T * K // E
    S = EL * C
    NU = D // U
    NQ = NU // 2
    NB = D // (2 * CW)
    NF = FF // U

    dd = lax.axis_index("data")
    oy = lax.axis_index("outer")
    jx = lax.axis_index("expert")
    cx = jx // 2
    cc = jx - 2 * cx
    nx = lax.axis_size("expert")

    def dev(r):
        ry, rx, rc = r // 4, (r // 2) % 2, r % 2
        y = 1 - oy if ry else oy
        x = 1 - cx if rx else cx
        c = 1 - cc if rc else cc
        return y, x * 2 + c

    def did(r):
        y, j = dev(r)
        return (dd, y, j)

    def pos_of(r):
        y, j = dev(r)
        return y * nx + j

    def xload(u):
        return pltpu.make_async_copy(x_hbm.at[:, pl.ds(u * U, U)], X.at[u * 8], xsem.at[u])

    wrload = pltpu.make_async_copy(wr_hbm, WR, xsem.at[NU])
    idxload = pltpu.make_async_copy(idx_hbm, IDX, xsem.at[NU + 1])

    def wtload(n, m):
        q, e, s = n // EL, n % EL, n % NWT
        src = w1_hbm if m == 0 else w3_hbm
        rows = pl.ds(pl.multiple_of(q * 2 * U, 2 * U), 2 * U)
        return pltpu.make_async_copy(src.at[e, rows, :], WT.at[s, m], wtsem.at[s, m])

    def w2load(n, m):
        b, e, s = n // EL, n % EL, n % NW2
        cols = pl.ds(pl.multiple_of(m * (D // 2) + b * CW, CW), CW)
        return pltpu.make_async_copy(w2_hbm.at[e, :, cols], W2T.at[s, :, pl.ds(m * CW, CW)], w2sem.at[s, m])

    H = T // 2

    def blk(u, r, half=None):
        b = u * 8 + r
        if half is None:
            return X.at[b]
        return X.at[b, pl.ds(half * H, H)]

    def disp(k, u):
        src, dst, to = [
            (blk(u, 0), blk(u, 2), 2), (blk(u, 0), blk(u, 4), 4), (blk(u, 0), blk(u, 1), 1),
            (blk(u, 2, 0), blk(u, 6, 0), 4), (blk(u, 4, 1), blk(u, 6, 1), 2),
            (blk(u, 2), blk(u, 3), 1), (blk(u, 4), blk(u, 5), 1), (blk(u, 6), blk(u, 7), 1),
        ][k]
        return pltpu.make_async_remote_copy(src_ref=src, dst_ref=dst, send_sem=dsend.at[k, u], recv_sem=drecv.at[k, u],
                                            device_id=did(to), device_id_type=MESH)

    def own(u):
        for k in (0, 1, 2):
            disp(k, u).start()

    def fwd(u):
        disp(0, u).wait_recv()
        disp(1, u).wait_recv()
        for k in (3, 4, 5, 6):
            disp(k, u).start()

    def diag(u):
        disp(3, u).wait_recv()
        disp(4, u).wait_recv()
        disp(7, u).start()

    def arrived(u):
        for k in (2, 5, 6, 7):
            disp(k, u).wait_recv()

    def sent(u):
        for k in range(8):
            disp(k, u).wait_send()

    def ecopy(r):
        rows = pl.ds(pl.multiple_of(pos_of(r) * EL, EL), EL)
        return pltpu.make_async_remote_copy(src_ref=ET.at[rows], dst_ref=EX.at[pl.ds(r * EL, EL)],
                                            send_sem=esend.at[r], recv_sem=erecv.at[r],
                                            device_id=did(r), device_id_type=MESH)

    for u in range(NU):
        xload(u).start()
    wrload.start()
    idxload.start()
    for n in range(NWT):
        wtload(n, 0).start()
        wtload(n, 1).start()

    barrier = pltpu.get_barrier_semaphore()
    for r in range(1, 8):
        pl.semaphore_signal(barrier, inc=1, device_id=did(r), device_id_type=MESH)
    xload(0).wait()
    pl.semaphore_wait(barrier, 7)
    own(0)

    for u in range(1, NU):
        xload(u).wait()
    wrload.wait()
    idxload.wait()
    logits = _dot(X[0], WR[0:U])
    for u in range(1, NU):
        logits = logits + _dot(X[u * 8], WR[u * U:(u + 1) * U])
    lane = lax.broadcasted_iota(jnp.int32, (T, E), 1)
    ids = IDX[...]
    chosen = lane == ids[:, 0:1]
    for j in range(1, K):
        chosen = chosen | (lane == ids[:, j:j + 1])
    top = jnp.max(jnp.where(chosen, logits, -jnp.inf), axis=1, keepdims=True)
    ex = jnp.where(chosen, jnp.exp(jnp.where(chosen, logits - top, 0.0)), 0.0)
    g = ex / jnp.sum(ex, axis=1, keepdims=True)
    ET[...] = jnp.transpose(jnp.where(chosen, g, -1.0))
    for r in range(1, 8):
        ecopy(r).start()
    own(1)

    @pl.loop(0, ACC.shape[0])
    def _(i):
        ACC[i] = jnp.zeros((U, U), F32)

    mine = pl.ds(pl.multiple_of(pos_of(0) * EL, EL), EL)
    EX[0:EL] = ET[mine]
    for r in range(1, 8):
        ecopy(r).wait_recv()

    ev = EX[...]
    sel = ev >= 0.0
    before = lax.broadcasted_iota(jnp.int32, (T, T), 0) < lax.broadcasted_iota(jnp.int32, (T, T), 1)
    cnt = _dot(sel.astype(F32).astype(BF), before.astype(F32).astype(BF))
    pos = jnp.where(sel, cnt, -1.0)
    POS[...] = pos

    @pl.loop(0, 8)
    def _(r):
        p = POS[pl.ds(pl.multiple_of(r * EL, EL), EL)]
        slot = lax.broadcasted_iota(jnp.int32, (C, T), 0).astype(F32)
        for e in range(EL):
            HT[r, e * C:(e + 1) * C, :] = jnp.where(jnp.broadcast_to(p[e:e + 1], (C, T)) == slot, 1.0, 0.0).astype(BF)

    fwd(0)
    own(2)

    ge = jnp.maximum(ev, 0.0)
    post = jnp.transpose(pos).astype(BF)
    gt = jnp.transpose(ge)
    hi = gt.astype(BF)
    rest = gt - hi.astype(F32)
    mid = rest.astype(BF)
    lo = (rest - mid.astype(F32)).astype(BF)

    @pl.loop(0, 8)
    def _(r):
        spread = jnp.where(lax.broadcasted_iota(jnp.int32, (8 * EL, S), 0)
                           == r * EL + lax.broadcasted_iota(jnp.int32, (8 * EL, S), 1) // C, 1.0, 0.0).astype(BF)
        slot = (lax.broadcasted_iota(jnp.int32, (T, S), 1) % C).astype(F32)
        hit = _dot(post, spread) == slot
        for k, part in enumerate((hi, mid, lo)):
            W[k * 8 + r] = jnp.where(hit, _dot(part, spread), 0.0).astype(BF)

    diag(0)
    fwd(1)
    own(3)
    arrived(0)
    diag(1)
    arrived(1)

    def gather(q):
        @pl.loop(0, 8)
        def _(r):
            rows = pl.ds(pl.multiple_of(r * C, C), C)
            for s in range(2):
                v = _dot(HT[r], X[(2 * q + s) * 8 + r])
                XIN[:, rows, s * U:(s + 1) * U] = v.astype(BF).reshape(EL, C, U)

    def tiles(n):
        wtload(n, 0).wait()
        wtload(n, 1).wait()

    @pl.loop(0, NQ - 1)
    def _(q):
        gather(q)

        @pl.loop(0, EL)
        def _(e):
            n = q * EL + e
            s = n % NWT
            tiles(n)
            xe = XIN[e]
            for m in range(2):
                for f in range(NF):
                    ACC[(e * 2 + m) * NF + f] += _dot(xe, WT[s, m, :, f * U:(f + 1) * U])
            for m in range(2):
                wtload(n + NWT, m).start()

            u = 2 * q + 2
            for at, step in ((2, lambda: fwd(u)), (6, lambda: diag(u)), (8, lambda: fwd(u + 1)), (12, lambda: diag(u + 1))):
                @pl.when(e == at)
                def _():
                    step()

            for at, k in ((2, 2), (8, 3)):
                @pl.when((e == at) & (u + k < NU))
                def _():
                    own(u + k)

        arrived(2 * q + 2)
        arrived(2 * q + 3)

    gather(NQ - 1)

    @pl.loop(0, NU)
    def _(u):
        sent(u)

    for r in range(1, 8):
        ecopy(r).wait_send()

    for n in range(NW2):
        w2load(n, 0).start()
        w2load(n, 1).start()

    @pl.loop(0, EL)
    def _(e):
        n = (NQ - 1) * EL + e
        s = n % NWT
        tiles(n)
        xe = XIN[e]
        for f in range(NF):
            a = ACC[e * 2 * NF + f] + _dot(xe, WT[s, 0, :, f * U:(f + 1) * U])
            b = ACC[(e * 2 + 1) * NF + f] + _dot(xe, WT[s, 1, :, f * U:(f + 1) * U])
            X[e * NF + f] = (jax.nn.silu(a) * b).astype(BF)

        @pl.when(n + NWT < NQ * EL)
        def _():
            for m in range(2):
                wtload(n + NWT, m).start()

    for r in (1, 2, 4):
        pl.semaphore_signal(ready, inc=1, device_id=did(r), device_id_type=MESH)

    R1 = 4 * NB
    R2 = R1 + 2 * NB
    YS = R2 + NB
    SS = YS + 8
    TT = SS + 12
    A = pl.ds(0, CW)
    B = pl.ds(CW, CW)

    def d2d(b):
        return pltpu.make_async_remote_copy(
            src_ref=ACC.at[pl.ds(YS + (b % 2) * 4, 4)], dst_ref=ACC.at[pl.ds(b * 4, 4)],
            send_sem=d2s.at[b], recv_sem=d2r.at[b], device_id=did(1), device_id_type=MESH)

    def hop1(b, k):
        src, dst, half, to = [(2, 0, A, 4), (3, 1, A, 4), (1, 0, B, 2), (3, 1, B, 2)][k]
        return pltpu.make_async_remote_copy(
            src_ref=ACC.at[SS + (b % 3) * 4 + src, :, half], dst_ref=ACC.at[R1 + b * 2 + dst, :, half],
            send_sem=p1s.at[b, k], recv_sem=p1r.at[b, k], device_id=did(to), device_id_type=MESH)

    def hop2(b, k):
        half, to = [(A, 2), (B, 4)][k]
        return pltpu.make_async_remote_copy(
            src_ref=ACC.at[TT + b % 2, :, half], dst_ref=ACC.at[R2 + b, :, half],
            send_sem=p2s.at[b, k], recv_sem=p2r.at[b, k], device_id=did(to), device_id_type=MESH)

    def combine(r):
        rows = slice(r * C, (r + 1) * C)
        o = OB[:, rows, :].reshape(S, 2 * CW)
        return _dot(W[r], o) + _dot(W[8 + r], o) + _dot(W[16 + r], o)

    @pl.loop(0, NB + 2)
    def _(b):
        @pl.when(b < NB)
        def _():
            @pl.loop(0, EL)
            def _(e):
                n = b * EL + e
                s = n % NW2
                w2load(n, 0).wait()
                w2load(n, 1).wait()
                h = jnp.concatenate([X[e * NF + f] for f in range(NF)], axis=1)
                OB[e] = _dot(h, W2T[s]).astype(BF)

                @pl.when(n + NW2 < NB * EL)
                def _():
                    w2load(n + NW2, 0).start()
                    w2load(n + NW2, 1).start()

            for i in range(4):
                ACC[YS + (b % 2) * 4 + i] = combine(2 * i + 1)

            @pl.when(b == 0)
            def _():
                pl.semaphore_wait(ready, 3)

            d2d(b).start()
            sb = SS + (b % 3) * 4
            for i in range(4):
                ACC[sb + i] = combine(2 * i)
            d2d(b).wait_recv()
            for i in (3, 2, 1, 0):
                ACC[sb + i] += ACC[b * 4 + i]
            for k in (1, 3, 0, 2):
                hop1(b, k).start()
            d2d(b).wait_send()

        c = b - 1

        @pl.when((c >= 0) & (c < NB))
        def _():
            sc = SS + (c % 3) * 4
            for k, i, half in ((1, 1, slice(0, CW)), (3, 2, slice(CW, 2 * CW))):
                hop1(c, k).wait_recv()
                ACC[TT + c % 2, :, half] = ACC[sc + i, :, half] + ACC[R1 + c * 2 + 1, :, half]
                hop2(c, (k - 1) // 2).start()
            for k in range(4):
                hop1(c, k).wait_send()

        f = b - 2

        @pl.when(f >= 0)
        def _():
            sf = SS + (f % 3) * 4
            hop1(f, 0).wait_recv()
            hop1(f, 2).wait_recv()
            for k, half in ((0, slice(0, CW)), (1, slice(CW, 2 * CW))):
                hop2(f, k).wait_recv()
                cols = pl.ds(pl.multiple_of(k * (D // 2) + f * CW, CW), CW)
                out_ref[:, cols] = (ACC[sf, :, half] + ACC[R1 + f * 2, :, half] + ACC[R2 + f, :, half]).astype(BF)
                hop2(f, k).wait_send()


def solution(mesh):
    tok = P(('data', 'outer', 'expert'), None)
    wsp = P(('outer', 'expert'), None, None)

    def local(x, wr, idx, w1, w3, w2):
        T, D = x.shape
        E = wr.shape[1]
        EL, _, FF = w1.shape
        K = idx.shape[1]
        C = 2 * T * K // E
        S = EL * C
        NU = D // U
        NB = D // (2 * CW)
        NF = FF // U
        any_ = pl.BlockSpec(memory_space=pl.ANY)
        dma = pltpu.SemaphoreType.DMA
        return pl.pallas_call(
            kernel,
            out_shape=jax.ShapeDtypeStruct((T, D), BF),
            in_specs=[any_] * 6,
            out_specs=pl.BlockSpec(memory_space=pltpu.VMEM),
            scratch_shapes=[
                pltpu.VMEM((NU * 8, T, U), BF),
                pltpu.VMEM((D, E), BF),
                pltpu.VMEM((T, K), jnp.int32),
                pltpu.VMEM((E, T), F32),
                pltpu.VMEM((8 * EL, T), F32),
                pltpu.VMEM((8 * EL, T), F32),
                pltpu.VMEM((8, S, T), BF),
                pltpu.VMEM((24, T, S), BF),
                pltpu.VMEM((EL, 8 * C, 2 * U), BF),
                pltpu.VMEM((EL * 2 * NF, 8 * C, U), F32),
                pltpu.VMEM((NWT, 2, 2 * U, FF), BF),
                pltpu.VMEM((NW2, FF, 2 * CW), BF),
                pltpu.VMEM((EL, 8 * C, 2 * CW), BF),
                dma((NU + 2,)), dma((NWT, 2)), dma((NW2, 2)),
                dma((8, NU)), dma((8, NU)), dma((8,)), dma((8,)),
                dma((NB,)), dma((NB,)), dma((NB, 4)), dma((NB, 4)), dma((NB, 2)), dma((NB, 2)),
                pltpu.SemaphoreType.REGULAR,
            ],
            compiler_params=pltpu.CompilerParams(collective_id=0, has_side_effects=True, vmem_limit_bytes=67043328),
        )(x, wr, idx, w1, w3, w2)

    return jax.shard_map(local, mesh=mesh, in_specs=(tok, P(None, None), tok, wsp, wsp, wsp), out_specs=tok, check_vma=False)
```

```python
import functools

import jax
import jax.numpy as jnp
from jax import lax
from jax.experimental import pallas as pl
from jax.experimental.pallas import tpu as pltpu
from jax.sharding import PartitionSpec as P

MESH = pl.DeviceIdType.MESH
BF = jnp.bfloat16
F32 = jnp.float32
U = 256
CW = 128
NWT = 6
NW2 = 10


def _dot(a, b):
    return jnp.dot(a, b, preferred_element_type=F32)


def kernel(x_hbm, wr_hbm, idx_hbm, w1_hbm, w3_hbm, w2_hbm, out_ref,
           X, WR, IDX, ET, EX, POS, HT, W, XIN, ACC, WT, W2T, OB,
           xsem, wtsem, w2sem, dsend, drecv, esend, erecv,
           d2s, d2r, p1s, p1r, p2s, p2r, ready):
    T, D = x_hbm.shape
    E = wr_hbm.shape[1]
    EL, _, FF = w1_hbm.shape
    K = idx_hbm.shape[0]
    C = 2 * T * K // E
    S = EL * C
    NU = D // U
    NQ = NU // 2
    NB = D // (2 * CW)
    NF = FF // U

    dd = lax.axis_index("data")
    oy = lax.axis_index("outer")
    jx = lax.axis_index("expert")
    cx = jx // 2
    cc = jx - 2 * cx
    nx = lax.axis_size("expert")

    def dev(r):
        ry, rx, rc = r // 4, (r // 2) % 2, r % 2
        y = 1 - oy if ry else oy
        x = 1 - cx if rx else cx
        c = 1 - cc if rc else cc
        return y, x * 2 + c

    def did(r):
        y, j = dev(r)
        return (dd, y, j)

    def pos_of(r):
        y, j = dev(r)
        return y * nx + j

    def xload(u):
        return pltpu.make_async_copy(x_hbm.at[:, pl.ds(u * U, U)], X.at[u * 8], xsem.at[u])

    wrload = pltpu.make_async_copy(wr_hbm, WR, xsem.at[NU])
    idxload = pltpu.make_async_copy(idx_hbm, IDX, xsem.at[NU + 1])

    def wtload(n, m):
        q, e, s = n // EL, n % EL, n % NWT
        src = w1_hbm if m == 0 else w3_hbm
        rows = pl.ds(pl.multiple_of(q * 2 * U, 2 * U), 2 * U)
        return pltpu.make_async_copy(src.at[e, rows, :], WT.at[s, m], wtsem.at[s, m])

    def w2load(n):
        b, e, s = n // EL, n % EL, n % NW2
        cols = pl.ds(pl.multiple_of(b * 2 * CW, 2 * CW), 2 * CW)
        return pltpu.make_async_copy(w2_hbm.at[e, :, cols], W2T.at[s], w2sem.at[s])

    H = T // 2

    def blk(u, r, half=None):
        b = u * 8 + r
        if half is None:
            return X.at[b]
        return X.at[b, pl.ds(half * H, H)]

    def disp(k, u):
        src, dst, to = [
            (blk(u, 0), blk(u, 2), 2), (blk(u, 0), blk(u, 4), 4), (blk(u, 0), blk(u, 1), 1),
            (blk(u, 2, 0), blk(u, 6, 0), 4), (blk(u, 4, 1), blk(u, 6, 1), 2),
            (blk(u, 2), blk(u, 3), 1), (blk(u, 4), blk(u, 5), 1), (blk(u, 6), blk(u, 7), 1),
        ][k]
        return pltpu.make_async_remote_copy(src_ref=src, dst_ref=dst, send_sem=dsend.at[k, u], recv_sem=drecv.at[k, u],
                                            device_id=did(to), device_id_type=MESH)

    def own(u):
        for k in (0, 1, 2):
            disp(k, u).start()

    def fwd(u):
        disp(0, u).wait_recv()
        disp(1, u).wait_recv()
        for k in (3, 4, 5, 6):
            disp(k, u).start()

    def diag(u):
        disp(3, u).wait_recv()
        disp(4, u).wait_recv()
        disp(7, u).start()

    def arrived(u):
        for k in (2, 5, 6, 7):
            disp(k, u).wait_recv()

    def sent(u):
        for k in range(8):
            disp(k, u).wait_send()

    def ecopy(r):
        rows = pl.ds(pl.multiple_of(pos_of(r) * EL, EL), EL)
        return pltpu.make_async_remote_copy(src_ref=ET.at[rows], dst_ref=EX.at[pl.ds(r * EL, EL)],
                                            send_sem=esend.at[r], recv_sem=erecv.at[r],
                                            device_id=did(r), device_id_type=MESH)

    for u in range(NU):
        xload(u).start()
    wrload.start()
    idxload.start()
    for n in range(NWT):
        wtload(n, 0).start()
        wtload(n, 1).start()

    barrier = pltpu.get_barrier_semaphore()
    for r in range(1, 8):
        pl.semaphore_signal(barrier, inc=1, device_id=did(r), device_id_type=MESH)
    xload(0).wait()
    pl.semaphore_wait(barrier, 7)
    own(0)

    for u in range(1, NU):
        xload(u).wait()
    wrload.wait()
    idxload.wait()
    logits = _dot(X[0], WR[0:U])
    for u in range(1, NU):
        logits = logits + _dot(X[u * 8], WR[u * U:(u + 1) * U])
    lane = lax.broadcasted_iota(jnp.int32, (T, E), 1)
    ids = jnp.transpose(IDX[...].astype(F32)).astype(jnp.int32)
    chosen = lane == ids[:, 0:1]
    for j in range(1, K):
        chosen = chosen | (lane == ids[:, j:j + 1])
    top = jnp.max(jnp.where(chosen, logits, -jnp.inf), axis=1, keepdims=True)
    ex = jnp.where(chosen, jnp.exp(jnp.where(chosen, logits - top, 0.0)), 0.0)
    g = ex / jnp.sum(ex, axis=1, keepdims=True)
    ET[...] = jnp.transpose(jnp.where(chosen, g, -1.0))
    for r in range(1, 8):
        ecopy(r).start()
    own(1)

    @pl.loop(0, ACC.shape[0])
    def _(i):
        ACC[i] = jnp.zeros((U, U), F32)

    mine = pl.ds(pl.multiple_of(pos_of(0) * EL, EL), EL)
    EX[0:EL] = ET[mine]
    for r in range(1, 8):
        ecopy(r).wait_recv()

    ev = EX[...]
    sel = ev >= 0.0
    before = lax.broadcasted_iota(jnp.int32, (T, T), 0) < lax.broadcasted_iota(jnp.int32, (T, T), 1)
    cnt = _dot(sel.astype(F32).astype(BF), before.astype(F32).astype(BF))
    pos = jnp.where(sel, cnt, -1.0)
    POS[...] = pos

    @pl.loop(0, 8)
    def _(r):
        p = POS[pl.ds(pl.multiple_of(r * EL, EL), EL)]
        slot = lax.broadcasted_iota(jnp.int32, (C, T), 0).astype(F32)
        for e in range(EL):
            HT[r, e * C:(e + 1) * C, :] = jnp.where(jnp.broadcast_to(p[e:e + 1], (C, T)) == slot, 1.0, 0.0).astype(BF)

    fwd(0)
    own(2)

    ge = jnp.maximum(ev, 0.0)
    post = jnp.transpose(pos).astype(BF)
    gt = jnp.transpose(ge)
    hi = gt.astype(BF)
    rest = gt - hi.astype(F32)
    mid = rest.astype(BF)
    lo = (rest - mid.astype(F32)).astype(BF)

    @pl.loop(0, 8)
    def _(r):
        spread = jnp.where(lax.broadcasted_iota(jnp.int32, (8 * EL, S), 0)
                           == r * EL + lax.broadcasted_iota(jnp.int32, (8 * EL, S), 1) // C, 1.0, 0.0).astype(BF)
        slot = (lax.broadcasted_iota(jnp.int32, (T, S), 1) % C).astype(F32)
        hit = _dot(post, spread) == slot
        for k, part in enumerate((hi, mid, lo)):
            W[k * 8 + r] = jnp.where(hit, _dot(part, spread), 0.0).astype(BF)

    diag(0)
    fwd(1)
    own(3)
    arrived(0)
    diag(1)
    arrived(1)

    def gather(q):
        @pl.loop(0, 8)
        def _(r):
            rows = pl.ds(pl.multiple_of(r * C, C), C)
            for s in range(2):
                v = _dot(HT[r], X[(2 * q + s) * 8 + r])
                XIN[:, rows, s * U:(s + 1) * U] = v.astype(BF).reshape(EL, C, U)

    def tiles(n):
        wtload(n, 0).wait()
        wtload(n, 1).wait()

    @pl.loop(0, NQ - 1)
    def _(q):
        gather(q)

        @pl.loop(0, EL)
        def _(e):
            n = q * EL + e
            s = n % NWT
            tiles(n)
            xe = XIN[e]
            for m in range(2):
                for f in range(NF):
                    ACC[(e * 2 + m) * NF + f] += _dot(xe, WT[s, m, :, f * U:(f + 1) * U])
            for m in range(2):
                wtload(n + NWT, m).start()

            u = 2 * q + 2
            for at, step in ((2, lambda: fwd(u)), (6, lambda: diag(u)), (8, lambda: fwd(u + 1)), (12, lambda: diag(u + 1))):
                @pl.when(e == at)
                def _():
                    step()

            for at, k in ((2, 2), (8, 3)):
                @pl.when((e == at) & (u + k < NU))
                def _():
                    own(u + k)

        arrived(2 * q + 2)
        arrived(2 * q + 3)

    gather(NQ - 1)

    @pl.loop(0, NU)
    def _(u):
        sent(u)

    for r in range(1, 8):
        ecopy(r).wait_send()

    for n in range(NW2):
        w2load(n).start()

    @pl.loop(0, EL)
    def _(e):
        n = (NQ - 1) * EL + e
        s = n % NWT
        tiles(n)
        xe = XIN[e]
        for f in range(NF):
            a = ACC[e * 2 * NF + f] + _dot(xe, WT[s, 0, :, f * U:(f + 1) * U])
            b = ACC[(e * 2 + 1) * NF + f] + _dot(xe, WT[s, 1, :, f * U:(f + 1) * U])
            X[e * NF + f] = (jax.nn.silu(a) * b).astype(BF)

        @pl.when(n + NWT < NQ * EL)
        def _():
            for m in range(2):
                wtload(n + NWT, m).start()

    for r in (1, 2, 4):
        pl.semaphore_signal(ready, inc=1, device_id=did(r), device_id_type=MESH)

    R1 = 4 * NB
    R2 = R1 + 2 * NB
    YS = R2 + NB
    SS = YS + 8
    TT = SS + 12
    A = pl.ds(0, CW)
    B = pl.ds(CW, CW)

    def d2d(b):
        return pltpu.make_async_remote_copy(
            src_ref=ACC.at[pl.ds(YS + (b % 2) * 4, 4)], dst_ref=ACC.at[pl.ds(b * 4, 4)],
            send_sem=d2s.at[b], recv_sem=d2r.at[b], device_id=did(1), device_id_type=MESH)

    def hop1(b, k):
        src, dst, half, to = [(2, 0, A, 4), (3, 1, A, 4), (1, 0, B, 2), (3, 1, B, 2)][k]
        return pltpu.make_async_remote_copy(
            src_ref=ACC.at[SS + (b % 3) * 4 + src, :, half], dst_ref=ACC.at[R1 + b * 2 + dst, :, half],
            send_sem=p1s.at[b, k], recv_sem=p1r.at[b, k], device_id=did(to), device_id_type=MESH)

    def hop2(b, k):
        half, to = [(A, 2), (B, 4)][k]
        return pltpu.make_async_remote_copy(
            src_ref=ACC.at[TT + b % 2, :, half], dst_ref=ACC.at[R2 + b, :, half],
            send_sem=p2s.at[b, k], recv_sem=p2r.at[b, k], device_id=did(to), device_id_type=MESH)

    def combine(r):
        rows = slice(r * C, (r + 1) * C)
        o = OB[:, rows, :].reshape(S, 2 * CW)
        return _dot(W[r], o) + _dot(W[8 + r], o) + _dot(W[16 + r], o)

    @pl.loop(0, NB + 2)
    def _(b):
        @pl.when(b < NB)
        def _():
            @pl.loop(0, EL)
            def _(e):
                n = b * EL + e
                s = n % NW2
                w2load(n).wait()
                h = jnp.concatenate([X[e * NF + f] for f in range(NF)], axis=1)
                OB[e] = _dot(h, W2T[s]).astype(BF)

                @pl.when(n + NW2 < NB * EL)
                def _():
                    w2load(n + NW2).start()

            for i in range(4):
                ACC[YS + (b % 2) * 4 + i] = combine(2 * i + 1)

            @pl.when(b == 0)
            def _():
                pl.semaphore_wait(ready, 3)

            d2d(b).start()
            sb = SS + (b % 3) * 4
            for i in range(4):
                ACC[sb + i] = combine(2 * i)
            d2d(b).wait_recv()
            for i in (3, 2, 1, 0):
                ACC[sb + i] += ACC[b * 4 + i]
            for k in (1, 3, 0, 2):
                hop1(b, k).start()
            d2d(b).wait_send()

        c = b - 1

        @pl.when((c >= 0) & (c < NB))
        def _():
            sc = SS + (c % 3) * 4
            for k, i, half in ((1, 1, slice(0, CW)), (3, 2, slice(CW, 2 * CW))):
                hop1(c, k).wait_recv()
                ACC[TT + c % 2, :, half] = ACC[sc + i, :, half] + ACC[R1 + c * 2 + 1, :, half]
                hop2(c, (k - 1) // 2).start()
            for k in range(4):
                hop1(c, k).wait_send()

        f = b - 2

        @pl.when(f >= 0)
        def _():
            sf = SS + (f % 3) * 4
            hop1(f, 0).wait_recv()
            hop1(f, 2).wait_recv()
            for k, half in ((0, slice(0, CW)), (1, slice(CW, 2 * CW))):
                hop2(f, k).wait_recv()
                cols = pl.ds(pl.multiple_of(f * 2 * CW + k * CW, CW), CW)
                out_ref[:, cols] = (ACC[sf, :, half] + ACC[R1 + f * 2, :, half] + ACC[R2 + f, :, half]).astype(BF)
                hop2(f, k).wait_send()


def solution(mesh):
    tok = P(('data', 'outer', 'expert'), None)
    wsp = P(('outer', 'expert'), None, None)

    def local(x, wr, idx, w1, w3, w2):
        T, D = x.shape
        E = wr.shape[1]
        EL, _, FF = w1.shape
        K = idx.shape[1]
        C = 2 * T * K // E
        S = EL * C
        NU = D // U
        NB = D // (2 * CW)
        NF = FF // U
        any_ = pl.BlockSpec(memory_space=pl.ANY)
        dma = pltpu.SemaphoreType.DMA
        return pl.pallas_call(
            kernel,
            out_shape=jax.ShapeDtypeStruct((T, D), BF),
            in_specs=[any_] * 6,
            out_specs=pl.BlockSpec(memory_space=pltpu.VMEM),
            scratch_shapes=[
                pltpu.VMEM((NU * 8, T, U), BF),
                pltpu.VMEM((D, E), BF),
                pltpu.VMEM((K, T), jnp.int32),
                pltpu.VMEM((E, T), F32),
                pltpu.VMEM((8 * EL, T), F32),
                pltpu.VMEM((8 * EL, T), F32),
                pltpu.VMEM((8, S, T), BF),
                pltpu.VMEM((24, T, S), BF),
                pltpu.VMEM((EL, 8 * C, 2 * U), BF),
                pltpu.VMEM((EL * 2 * NF, 8 * C, U), F32),
                pltpu.VMEM((NWT, 2, 2 * U, FF), BF),
                pltpu.VMEM((NW2, FF, 2 * CW), BF),
                pltpu.VMEM((EL, 8 * C, 2 * CW), BF),
                dma((NU + 2,)), dma((NWT, 2)), dma((NW2,)),
                dma((8, NU)), dma((8, NU)), dma((8,)), dma((8,)),
                dma((NB,)), dma((NB,)), dma((NB, 4)), dma((NB, 4)), dma((NB, 2)), dma((NB, 2)),
                pltpu.SemaphoreType.REGULAR,
            ],
            compiler_params=pltpu.CompilerParams(collective_id=0, has_side_effects=True, vmem_limit_bytes=67043328),
        )(x, wr, idx.T, w1, w3, w2)

    return jax.shard_map(local, mesh=mesh, in_specs=(tok, P(None, None), tok, wsp, wsp, wsp), out_specs=tok, check_vma=False)
```

```python
import functools

import jax
import jax.numpy as jnp
from jax import lax
from jax.experimental import pallas as pl
from jax.experimental.pallas import tpu as pltpu
from jax.sharding import PartitionSpec as P

MESH = pl.DeviceIdType.MESH
BF = jnp.bfloat16
F32 = jnp.float32
U = 256
CW = 128
NWT = 8
UE = 4


def _dot(a, b):
    return jnp.dot(a, b, preferred_element_type=F32)


def kernel(x_hbm, wr_hbm, idx_hbm, w1_hbm, w3_hbm, w2_hbm, out_ref,
           X, WR, IDX, ET, EX, POS, HT, W, XIN, ACC, WT,
           xsem, wtsem, w2sem, dsend, drecv, esend, erecv,
           d2s, d2r, p1s, p1r, p2s, p2r, ready):
    T, D = x_hbm.shape
    E = wr_hbm.shape[1]
    EL, _, FF = w1_hbm.shape
    K = idx_hbm.shape[0]
    C = 2 * T * K // E
    S = EL * C
    NU = D // U
    NQ = NU // 2
    NB = D // (2 * CW)
    NF = FF // U

    dd = lax.axis_index("data")
    oy = lax.axis_index("outer")
    jx = lax.axis_index("expert")
    cx = jx // 2
    cc = jx - 2 * cx
    nx = lax.axis_size("expert")

    def dev(r):
        ry, rx, rc = r // 4, (r // 2) % 2, r % 2
        y = 1 - oy if ry else oy
        x = 1 - cx if rx else cx
        c = 1 - cc if rc else cc
        return y, x * 2 + c

    def did(r):
        y, j = dev(r)
        return (dd, y, j)

    def pos_of(r):
        y, j = dev(r)
        return y * nx + j

    def xload(u):
        return pltpu.make_async_copy(x_hbm.at[:, pl.ds(u * U, U)], X.at[u * 8], xsem.at[u])

    wrload = pltpu.make_async_copy(wr_hbm, WR, xsem.at[NU])
    idxload = pltpu.make_async_copy(idx_hbm, IDX, xsem.at[NU + 1])

    def wtload(n, m):
        q, e, s = n // EL, n % EL, n % NWT
        src = w1_hbm if m == 0 else w3_hbm
        rows = pl.ds(pl.multiple_of(q * 2 * U, 2 * U), 2 * U)
        return pltpu.make_async_copy(src.at[e, rows, :], WT.at[s, m], wtsem.at[s, m])

    R = 2 * U

    def w2load(b, e):
        cols = pl.ds(pl.multiple_of(b * 2 * CW, 2 * CW), 2 * CW)
        s, m = e // 2, e % 2
        return (
            pltpu.make_async_copy(w2_hbm.at[e, 0:R, cols], WT.at[s, m, :, 0:2 * CW], w2sem.at[e, 0]),
            pltpu.make_async_copy(w2_hbm.at[e, R:FF, cols], WT.at[s, m, 0:FF - R, 2 * CW:4 * CW], w2sem.at[e, 1]))

    def w2start(b, e):
        for c in w2load(b, e):
            c.start()

    def w2tile(e):
        s, m = e // 2, e % 2
        return jnp.concatenate([WT[s, m, :, 0:2 * CW], WT[s, m, 0:FF - R, 2 * CW:4 * CW]], axis=0)

    H = T // 2

    def blk(u, r, half=None):
        b = u * 8 + r
        if half is None:
            return X.at[b]
        return X.at[b, pl.ds(half * H, H)]

    def disp(k, u):
        src, dst, to = [
            (blk(u, 0), blk(u, 2), 2), (blk(u, 0), blk(u, 4), 4), (blk(u, 0), blk(u, 1), 1),
            (blk(u, 2, 0), blk(u, 6, 0), 4), (blk(u, 4, 1), blk(u, 6, 1), 2),
            (blk(u, 2), blk(u, 3), 1), (blk(u, 4), blk(u, 5), 1), (blk(u, 6), blk(u, 7), 1),
        ][k]
        return pltpu.make_async_remote_copy(src_ref=src, dst_ref=dst, send_sem=dsend.at[k, u], recv_sem=drecv.at[k, u],
                                            device_id=did(to), device_id_type=MESH)

    def own(u):
        for k in (0, 1, 2):
            disp(k, u).start()

    def fwd(u):
        disp(0, u).wait_recv()
        disp(1, u).wait_recv()
        for k in (3, 4, 5, 6):
            disp(k, u).start()

    def diag(u):
        disp(3, u).wait_recv()
        disp(4, u).wait_recv()
        disp(7, u).start()

    def arrived(u):
        for k in (2, 5, 6, 7):
            disp(k, u).wait_recv()

    def sent(u):
        for k in range(8):
            disp(k, u).wait_send()

    def ecopy(r):
        rows = pl.ds(pl.multiple_of(pos_of(r) * EL, EL), EL)
        return pltpu.make_async_remote_copy(src_ref=ET.at[rows], dst_ref=EX.at[pl.ds(r * EL, EL)],
                                            send_sem=esend.at[r], recv_sem=erecv.at[r],
                                            device_id=did(r), device_id_type=MESH)

    for u in range(NU):
        xload(u).start()
    wrload.start()
    idxload.start()
    for n in range(NWT):
        wtload(n, 0).start()
        wtload(n, 1).start()

    barrier = pltpu.get_barrier_semaphore()
    for r in range(1, 8):
        pl.semaphore_signal(barrier, inc=1, device_id=did(r), device_id_type=MESH)
    xload(0).wait()
    pl.semaphore_wait(barrier, 7)
    own(0)

    for u in range(1, NU):
        xload(u).wait()
    wrload.wait()
    idxload.wait()
    logits = _dot(X[0], WR[0:U])
    for u in range(1, NU):
        logits = logits + _dot(X[u * 8], WR[u * U:(u + 1) * U])
    lane = lax.broadcasted_iota(jnp.int32, (T, E), 1)
    ids = jnp.transpose(IDX[...].astype(F32)).astype(jnp.int32)
    chosen = lane == ids[:, 0:1]
    for j in range(1, K):
        chosen = chosen | (lane == ids[:, j:j + 1])
    top = jnp.max(jnp.where(chosen, logits, -jnp.inf), axis=1, keepdims=True)
    ex = jnp.where(chosen, jnp.exp(jnp.where(chosen, logits - top, 0.0)), 0.0)
    g = ex / jnp.sum(ex, axis=1, keepdims=True)
    ET[...] = jnp.transpose(jnp.where(chosen, g, -1.0))
    for r in range(1, 8):
        ecopy(r).start()
    own(1)

    @pl.loop(0, ACC.shape[0])
    def _(i):
        ACC[i] = jnp.zeros((U, U), F32)

    mine = pl.ds(pl.multiple_of(pos_of(0) * EL, EL), EL)
    EX[0:EL] = ET[mine]
    for r in range(1, 8):
        ecopy(r).wait_recv()

    ev = EX[...]
    sel = ev >= 0.0
    before = lax.broadcasted_iota(jnp.int32, (T, T), 0) < lax.broadcasted_iota(jnp.int32, (T, T), 1)
    cnt = _dot(sel.astype(F32).astype(BF), before.astype(F32).astype(BF))
    pos = jnp.where(sel, cnt, -1.0)
    POS[...] = pos

    @pl.loop(0, 8)
    def _(r):
        p = POS[pl.ds(pl.multiple_of(r * EL, EL), EL)]
        slot = lax.broadcasted_iota(jnp.int32, (C, T), 0).astype(F32)
        for e in range(EL):
            HT[r, e * C:(e + 1) * C, :] = jnp.where(jnp.broadcast_to(p[e:e + 1], (C, T)) == slot, 1.0, 0.0).astype(BF)

    fwd(0)
    own(2)

    ge = jnp.maximum(ev, 0.0)
    post = jnp.transpose(pos).astype(BF)
    gt = jnp.transpose(ge)
    hi = gt.astype(BF)
    rest = gt - hi.astype(F32)
    mid = rest.astype(BF)
    lo = (rest - mid.astype(F32)).astype(BF)

    @pl.loop(0, 8)
    def _(r):
        spread = jnp.where(lax.broadcasted_iota(jnp.int32, (8 * EL, S), 0)
                           == r * EL + lax.broadcasted_iota(jnp.int32, (8 * EL, S), 1) // C, 1.0, 0.0).astype(BF)
        slot = (lax.broadcasted_iota(jnp.int32, (T, S), 1) % C).astype(F32)
        hit = _dot(post, spread) == slot
        for k, part in enumerate((hi, mid, lo)):
            W[k * 8 + r] = jnp.where(hit, _dot(part, spread), 0.0).astype(BF)

    diag(0)
    fwd(1)
    own(3)
    arrived(0)
    diag(1)
    arrived(1)

    def gather(q):
        @pl.loop(0, 2)
        def _(g):
            for i in range(4):
                r = g * 4 + i
                rows = pl.ds(pl.multiple_of(r * C, C), C)
                for s in range(2):
                    v = _dot(HT[r], X[(2 * q + s) * 8 + r])
                    XIN[:, rows, s * U:(s + 1) * U] = v.astype(BF).reshape(EL, C, U)

    def tiles(n):
        for i in range(UE):
            for m in range(2):
                wtload(n + i, m).wait()

    @pl.loop(0, NQ - 1)
    def _(q):
        u = 2 * q + 2
        fwd(u)

        @pl.when(u + 2 < NU)
        def _():
            own(u + 2)

        gather(q)

        @pl.loop(0, EL // UE)
        def _(g):
            n = q * EL + g * UE
            tiles(n)
            for i in range(UE):
                e, s = g * UE + i, (n + i) % NWT
                xe = XIN[e]
                for m in range(2):
                    for f in range(NF):
                        ACC[(e * 2 + m) * NF + f] += _dot(xe, WT[s, m, :, f * U:(f + 1) * U])
            for i in range(UE):
                for m in range(2):
                    wtload(n + NWT + i, m).start()

            @pl.when(g == 0)
            def _():
                diag(u)

            @pl.when(g == 1)
            def _():
                fwd(u + 1)

                @pl.when(u + 3 < NU)
                def _():
                    own(u + 3)

            @pl.when(g == 2)
            def _():
                diag(u + 1)

        arrived(u)
        arrived(u + 1)

    gather(NQ - 1)

    @pl.loop(0, NU)
    def _(u):
        sent(u)

    for r in range(1, 8):
        ecopy(r).wait_send()

    @pl.loop(0, EL // UE)
    def _(g):
        n = (NQ - 1) * EL + g * UE
        tiles(n)
        for i in range(UE):
            e, s = g * UE + i, (n + i) % NWT
            xe = XIN[e]
            for f in range(NF):
                a = ACC[e * 2 * NF + f] + _dot(xe, WT[s, 0, :, f * U:(f + 1) * U])
                b = ACC[(e * 2 + 1) * NF + f] + _dot(xe, WT[s, 1, :, f * U:(f + 1) * U])
                X[e * NF + f] = (jax.nn.silu(a) * b).astype(BF)

        @pl.when(n + NWT < NQ * EL)
        def _():
            for i in range(UE):
                for m in range(2):
                    wtload(n + NWT + i, m).start()

        @pl.when(n + NWT >= NQ * EL)
        def _():
            for i in range(2 * UE):
                w2start(0, (g - (EL // UE - 2)) * 2 * UE + i)

    for r in (1, 2, 4):
        pl.semaphore_signal(ready, inc=1, device_id=did(r), device_id_type=MESH)

    R1 = 4 * NB
    R2 = R1 + 2 * NB
    YS = R2 + NB
    SS = YS + 8
    TT = SS + 12
    A = pl.ds(0, CW)
    B = pl.ds(CW, CW)

    def d2d(b):
        return pltpu.make_async_remote_copy(
            src_ref=ACC.at[pl.ds(YS + (b % 2) * 4, 4)], dst_ref=ACC.at[pl.ds(b * 4, 4)],
            send_sem=d2s.at[b], recv_sem=d2r.at[b], device_id=did(1), device_id_type=MESH)

    def hop1(b, k):
        src, dst, half, to = [(2, 0, A, 4), (3, 1, A, 4), (1, 0, B, 2), (3, 1, B, 2)][k]
        return pltpu.make_async_remote_copy(
            src_ref=ACC.at[SS + (b % 3) * 4 + src, :, half], dst_ref=ACC.at[R1 + b * 2 + dst, :, half],
            send_sem=p1s.at[b, k], recv_sem=p1r.at[b, k], device_id=did(to), device_id_type=MESH)

    def hop2(b, k):
        half, to = [(A, 2), (B, 4)][k]
        return pltpu.make_async_remote_copy(
            src_ref=ACC.at[TT + b % 2, :, half], dst_ref=ACC.at[R2 + b, :, half],
            send_sem=p2s.at[b, k], recv_sem=p2r.at[b, k], device_id=did(to), device_id_type=MESH)

    def combine(r):
        rows = slice(r * C, (r + 1) * C)
        o = XIN[:, rows, 0:2 * CW].reshape(S, 2 * CW)
        return _dot(W[r], o) + _dot(W[8 + r], o) + _dot(W[16 + r], o)

    @pl.loop(0, NB + 2)
    def _(b):
        @pl.when(b < NB)
        def _():
            @pl.loop(0, EL // UE)
            def _(g):
                for i in range(UE):
                    for c in w2load(b, g * UE + i):
                        c.wait()
                for i in range(UE):
                    e = g * UE + i
                    h = jnp.concatenate([X[e * NF + f] for f in range(NF)], axis=1)
                    XIN[e, :, 0:2 * CW] = _dot(h, w2tile(e)).astype(BF)

                @pl.when(b + 1 < NB)
                def _():
                    for i in range(UE):
                        w2start(b + 1, g * UE + i)

            for i in range(4):
                ACC[YS + (b % 2) * 4 + i] = combine(2 * i + 1)

            @pl.when(b == 0)
            def _():
                pl.semaphore_wait(ready, 3)

            d2d(b).start()
            sb = SS + (b % 3) * 4
            for i in range(4):
                ACC[sb + i] = combine(2 * i)
            d2d(b).wait_recv()
            for i in (3, 2, 1, 0):
                ACC[sb + i] += ACC[b * 4 + i]
            for k in (1, 3, 0, 2):
                hop1(b, k).start()
            d2d(b).wait_send()

        c = b - 1

        @pl.when((c >= 0) & (c < NB))
        def _():
            sc = SS + (c % 3) * 4
            for k, i, half in ((1, 1, slice(0, CW)), (3, 2, slice(CW, 2 * CW))):
                hop1(c, k).wait_recv()
                ACC[TT + c % 2, :, half] = ACC[sc + i, :, half] + ACC[R1 + c * 2 + 1, :, half]
                hop2(c, (k - 1) // 2).start()
            for k in range(4):
                hop1(c, k).wait_send()

        f = b - 2

        @pl.when(f >= 0)
        def _():
            sf = SS + (f % 3) * 4
            hop1(f, 0).wait_recv()
            hop1(f, 2).wait_recv()
            for k, half in ((0, slice(0, CW)), (1, slice(CW, 2 * CW))):
                hop2(f, k).wait_recv()
                cols = pl.ds(pl.multiple_of(f * 2 * CW + k * CW, CW), CW)
                out_ref[:, cols] = (ACC[sf, :, half] + ACC[R1 + f * 2, :, half] + ACC[R2 + f, :, half]).astype(BF)
                hop2(f, k).wait_send()


def solution(mesh):
    tok = P(('data', 'outer', 'expert'), None)
    wsp = P(('outer', 'expert'), None, None)

    def local(x, wr, idx, w1, w3, w2):
        T, D = x.shape
        E = wr.shape[1]
        EL, _, FF = w1.shape
        K = idx.shape[1]
        C = 2 * T * K // E
        S = EL * C
        NU = D // U
        NB = D // (2 * CW)
        NF = FF // U
        any_ = pl.BlockSpec(memory_space=pl.ANY)
        dma = pltpu.SemaphoreType.DMA
        return pl.pallas_call(
            kernel,
            out_shape=jax.ShapeDtypeStruct((T, D), BF),
            in_specs=[any_] * 6,
            out_specs=pl.BlockSpec(memory_space=pltpu.VMEM),
            scratch_shapes=[
                pltpu.VMEM((NU * 8, T, U), BF),
                pltpu.VMEM((D, E), BF),
                pltpu.VMEM((K, T), jnp.int32),
                pltpu.VMEM((E, T), F32),
                pltpu.VMEM((8 * EL, T), F32),
                pltpu.VMEM((8 * EL, T), F32),
                pltpu.VMEM((8, S, T), BF),
                pltpu.VMEM((24, T, S), BF),
                pltpu.VMEM((EL, 8 * C, 2 * U), BF),
                pltpu.VMEM((EL * 2 * NF, 8 * C, U), F32),
                pltpu.VMEM((NWT, 2, 2 * U, FF), BF),
                dma((NU + 2,)), dma((NWT, 2)), dma((EL, 2)),
                dma((8, NU)), dma((8, NU)), dma((8,)), dma((8,)),
                dma((NB,)), dma((NB,)), dma((NB, 4)), dma((NB, 4)), dma((NB, 2)), dma((NB, 2)),
                pltpu.SemaphoreType.REGULAR,
            ],
            compiler_params=pltpu.CompilerParams(collective_id=0, has_side_effects=True, vmem_limit_bytes=67043328),
        )(x, wr, idx.T, w1, w3, w2)

    return jax.shard_map(local, mesh=mesh, in_specs=(tok, P(None, None), tok, wsp, wsp, wsp), out_specs=tok, check_vma=False)
```

```python
import functools

import jax
import jax.numpy as jnp
from jax import lax
from jax.experimental import pallas as pl
from jax.experimental.pallas import tpu as pltpu
from jax.sharding import PartitionSpec as P

MESH = pl.DeviceIdType.MESH
BF = jnp.bfloat16
F32 = jnp.float32
U = 256
CW = 128
NWT = 12
UE = 4


def _dot(a, b):
    return jnp.dot(a, b, preferred_element_type=F32)


def kernel(x_hbm, wr_hbm, idx_hbm, w1_hbm, w3_hbm, w2_hbm, out_hbm,
           X, IDX, ET, EX, POS, HT, W, XIN, ACC, WT,
           xsem, wtsem, w2sem, dsend, drecv, esend, erecv,
           d2s, d2r, p1s, p1r, p2s, p2r, osem, ready):
    T, D = x_hbm.shape
    E = wr_hbm.shape[1]
    EL, _, FF = w1_hbm.shape
    K = idx_hbm.shape[0]
    C = 2 * T * K // E
    S = EL * C
    NU = D // U
    NQ = NU // 2
    NB = D // (2 * CW)
    NF = FF // U

    dd = lax.axis_index("data")
    oy = lax.axis_index("outer")
    jx = lax.axis_index("expert")
    cx = jx // 2
    cc = jx - 2 * cx
    nx = lax.axis_size("expert")

    def dev(r):
        ry, rx, rc = r // 4, (r // 2) % 2, r % 2
        y = 1 - oy if ry else oy
        x = 1 - cx if rx else cx
        c = 1 - cc if rc else cc
        return y, x * 2 + c

    def did(r):
        y, j = dev(r)
        return (dd, y, j)

    def pos_of(r):
        y, j = dev(r)
        return y * nx + j

    def xload(u):
        return pltpu.make_async_copy(x_hbm.at[:, pl.ds(u * U, U)], X.at[u * 8], xsem.at[u])

    def wrload(u):
        return pltpu.make_async_copy(wr_hbm.at[pl.ds(u * U, U)], XIN.at[u, :, 0:E], xsem.at[NU + u])

    idxload = pltpu.make_async_copy(idx_hbm, IDX, xsem.at[2 * NU])

    def wtload(n, m):
        q, e, s = n // EL, n % EL, n % NWT
        src = w1_hbm if m == 0 else w3_hbm
        rows = pl.ds(pl.multiple_of(q * 2 * U, 2 * U), 2 * U)
        return pltpu.make_async_copy(src.at[e, rows, :], WT.at[s, m], wtsem.at[s, m])

    R = 2 * U

    def w2load(b, e):
        cols = pl.ds(pl.multiple_of(b * 2 * CW, 2 * CW), 2 * CW)
        s, m = NWT - EL // 2 + e // 2, e % 2
        return (
            pltpu.make_async_copy(w2_hbm.at[e, 0:R, cols], WT.at[s, m, :, 0:2 * CW], w2sem.at[e, 0]),
            pltpu.make_async_copy(w2_hbm.at[e, R:FF, cols], WT.at[s, m, 0:FF - R, 2 * CW:4 * CW], w2sem.at[e, 1]))

    def w2start(b, e):
        for c in w2load(b, e):
            c.start()

    def w2tile(e):
        s, m = NWT - EL // 2 + e // 2, e % 2
        return jnp.concatenate([WT[s, m, :, 0:2 * CW], WT[s, m, 0:FF - R, 2 * CW:4 * CW]], axis=0)

    H = T // 2

    def blk(u, r, half=None):
        b = u * 8 + r
        if half is None:
            return X.at[b]
        return X.at[b, pl.ds(half * H, H)]

    def disp(k, u):
        src, dst, to = [
            (blk(u, 0), blk(u, 2), 2), (blk(u, 0), blk(u, 4), 4), (blk(u, 0), blk(u, 1), 1),
            (blk(u, 2, 0), blk(u, 6, 0), 4), (blk(u, 4, 1), blk(u, 6, 1), 2),
            (blk(u, 2), blk(u, 3), 1), (blk(u, 4), blk(u, 5), 1), (blk(u, 6), blk(u, 7), 1),
        ][k]
        return pltpu.make_async_remote_copy(src_ref=src, dst_ref=dst, send_sem=dsend.at[k, u], recv_sem=drecv.at[k, u],
                                            device_id=did(to), device_id_type=MESH)

    def own(u):
        for k in (0, 1, 2):
            disp(k, u).start()

    def fwd(u):
        disp(0, u).wait_recv()
        disp(1, u).wait_recv()
        for k in (3, 4, 5, 6):
            disp(k, u).start()

    def diag(u):
        disp(3, u).wait_recv()
        disp(4, u).wait_recv()
        disp(7, u).start()

    def arrived(u):
        for k in (2, 5, 6, 7):
            disp(k, u).wait_recv()

    def sent(u):
        for k in range(8):
            disp(k, u).wait_send()

    def ecopy(r):
        rows = pl.ds(pl.multiple_of(pos_of(r) * EL, EL), EL)
        return pltpu.make_async_remote_copy(src_ref=ET.at[rows], dst_ref=EX.at[pl.ds(r * EL, EL)],
                                            send_sem=esend.at[r], recv_sem=erecv.at[r],
                                            device_id=did(r), device_id_type=MESH)

    for u in range(NU):
        xload(u).start()
    for u in range(NU):
        wrload(u).start()
    idxload.start()
    for n in range(NWT):
        wtload(n, 0).start()
        wtload(n, 1).start()

    barrier = pltpu.get_barrier_semaphore()
    for r in range(1, 8):
        pl.semaphore_signal(barrier, inc=1, device_id=did(r), device_id_type=MESH)
    xload(0).wait()
    pl.semaphore_wait(barrier, 7)
    own(0)

    for u in range(1, NU):
        xload(u).wait()
    for u in range(NU):
        wrload(u).wait()
    idxload.wait()
    logits = _dot(X[0], XIN[0, :, 0:E])
    for u in range(1, NU):
        logits = logits + _dot(X[u * 8], XIN[u, :, 0:E])
    lane = lax.broadcasted_iota(jnp.int32, (T, E), 1)
    ids = jnp.transpose(IDX[...].astype(F32)).astype(jnp.int32)
    chosen = lane == ids[:, 0:1]
    for j in range(1, K):
        chosen = chosen | (lane == ids[:, j:j + 1])
    top = jnp.max(jnp.where(chosen, logits, -jnp.inf), axis=1, keepdims=True)
    ex = jnp.where(chosen, jnp.exp(jnp.where(chosen, logits - top, 0.0)), 0.0)
    g = ex / jnp.sum(ex, axis=1, keepdims=True)
    ET[...] = jnp.transpose(jnp.where(chosen, g, -1.0))
    for r in range(1, 8):
        ecopy(r).start()
    own(1)

    @pl.loop(0, ACC.shape[0])
    def _(i):
        ACC[i] = jnp.zeros((U, U), F32)

    mine = pl.ds(pl.multiple_of(pos_of(0) * EL, EL), EL)
    EX[0:EL] = ET[mine]
    for r in range(1, 8):
        ecopy(r).wait_recv()

    ev = EX[...]
    sel = ev >= 0.0
    before = lax.broadcasted_iota(jnp.int32, (T, T), 0) < lax.broadcasted_iota(jnp.int32, (T, T), 1)
    cnt = _dot(sel.astype(F32).astype(BF), before.astype(F32).astype(BF))
    pos = jnp.where(sel, cnt, -1.0)
    POS[...] = pos

    @pl.loop(0, 8)
    def _(r):
        p = POS[pl.ds(pl.multiple_of(r * EL, EL), EL)]
        slot = lax.broadcasted_iota(jnp.int32, (C, T), 0).astype(F32)
        for e in range(EL):
            HT[r, e * C:(e + 1) * C, :] = jnp.where(jnp.broadcast_to(p[e:e + 1], (C, T)) == slot, 1.0, 0.0).astype(BF)

    fwd(0)
    own(2)

    ge = jnp.maximum(ev, 0.0)
    post = jnp.transpose(pos).astype(BF)
    gt = jnp.transpose(ge)
    hi = gt.astype(BF)
    rest = gt - hi.astype(F32)
    mid = rest.astype(BF)
    lo = (rest - mid.astype(F32)).astype(BF)

    @pl.loop(0, 8)
    def _(r):
        spread = jnp.where(lax.broadcasted_iota(jnp.int32, (8 * EL, S), 0)
                           == r * EL + lax.broadcasted_iota(jnp.int32, (8 * EL, S), 1) // C, 1.0, 0.0).astype(BF)
        slot = (lax.broadcasted_iota(jnp.int32, (T, S), 1) % C).astype(F32)
        hit = _dot(post, spread) == slot
        for k, part in enumerate((hi, mid, lo)):
            W[k * 8 + r] = jnp.where(hit, _dot(part, spread), 0.0).astype(BF)

    diag(0)
    fwd(1)
    own(3)
    arrived(0)
    diag(1)
    arrived(1)

    def gather(q):
        @pl.loop(0, 2)
        def _(g):
            for i in range(4):
                r = g * 4 + i
                rows = pl.ds(pl.multiple_of(r * C, C), C)
                for s in range(2):
                    v = _dot(HT[r], X[(2 * q + s) * 8 + r])
                    XIN[:, rows, s * U:(s + 1) * U] = v.astype(BF).reshape(EL, C, U)

    def tiles(n):
        for i in range(UE):
            for m in range(2):
                wtload(n + i, m).wait()

    @pl.loop(0, NQ - 1)
    def _(q):
        u = 2 * q + 2
        fwd(u)

        @pl.when(u + 2 < NU)
        def _():
            own(u + 2)

        gather(q)

        @pl.loop(0, EL // UE)
        def _(g):
            n = q * EL + g * UE
            tiles(n)
            for i in range(UE):
                e, s = g * UE + i, n % NWT + i
                xe = XIN[e]
                for m in range(2):
                    for f in range(NF):
                        ACC[(e * 2 + m) * NF + f] += _dot(xe, WT[s, m, :, f * U:(f + 1) * U])
            for i in range(UE):
                for m in range(2):
                    wtload(n + NWT + i, m).start()

            @pl.when(g == 0)
            def _():
                diag(u)

            @pl.when(g == 1)
            def _():
                fwd(u + 1)

                @pl.when(u + 3 < NU)
                def _():
                    own(u + 3)

            @pl.when(g == 2)
            def _():
                diag(u + 1)

        arrived(u)
        arrived(u + 1)

    gather(NQ - 1)

    @pl.loop(0, NU)
    def _(u):
        sent(u)

    for r in range(1, 8):
        ecopy(r).wait_send()

    @pl.loop(0, EL // UE)
    def _(g):
        n = (NQ - 1) * EL + g * UE
        tiles(n)
        for i in range(UE):
            e, s = g * UE + i, n % NWT + i
            xe = XIN[e]
            for f in range(NF):
                a = ACC[e * 2 * NF + f] + _dot(xe, WT[s, 0, :, f * U:(f + 1) * U])
                b = ACC[(e * 2 + 1) * NF + f] + _dot(xe, WT[s, 1, :, f * U:(f + 1) * U])
                X[e * NF + f] = (jax.nn.silu(a) * b).astype(BF)

        @pl.when(n + NWT < NQ * EL)
        def _():
            for i in range(UE):
                for m in range(2):
                    wtload(n + NWT + i, m).start()

        @pl.when((g == 1) | (g == 2))
        def _():
            for i in range(2 * UE):
                w2start(0, (g - 1) * 2 * UE + i)

    for r in (1, 2, 4):
        pl.semaphore_signal(ready, inc=1, device_id=did(r), device_id_type=MESH)

    R1 = 4 * NB
    R2 = R1 + 2 * NB
    YS = R2 + NB
    SS = YS + 8
    TT = SS + 12
    OUT = EL * NF

    def store(b):
        cols = pl.ds(pl.multiple_of(b * 2 * CW, 2 * CW), 2 * CW)
        return pltpu.make_async_copy(X.at[OUT + b], out_hbm.at[:, cols], osem.at[b])

    A = pl.ds(0, CW)
    B = pl.ds(CW, CW)

    def d2d(b, i):
        return pltpu.make_async_remote_copy(
            src_ref=ACC.at[YS + (b % 2) * 4 + i], dst_ref=ACC.at[b * 4 + i],
            send_sem=d2s.at[b, i], recv_sem=d2r.at[b, i], device_id=did(1), device_id_type=MESH)

    def hop1(b, k):
        src, dst, half, to = [(2, 0, A, 4), (3, 1, A, 4), (1, 0, B, 2), (3, 1, B, 2)][k]
        return pltpu.make_async_remote_copy(
            src_ref=ACC.at[SS + (b % 3) * 4 + src, :, half], dst_ref=ACC.at[R1 + b * 2 + dst, :, half],
            send_sem=p1s.at[b, k], recv_sem=p1r.at[b, k], device_id=did(to), device_id_type=MESH)

    def hop2(b, k):
        half, to = [(A, 2), (B, 4)][k]
        return pltpu.make_async_remote_copy(
            src_ref=ACC.at[TT + b % 2, :, half], dst_ref=ACC.at[R2 + b, :, half],
            send_sem=p2s.at[b, k], recv_sem=p2r.at[b, k], device_id=did(to), device_id_type=MESH)

    def combine(r):
        rows = slice(r * C, (r + 1) * C)
        o = XIN[:, rows, 0:2 * CW].reshape(S, 2 * CW)
        return _dot(W[r], o) + _dot(W[8 + r], o) + _dot(W[16 + r], o)

    @pl.loop(0, NB + 2)
    def _(b):
        @pl.when(b < NB)
        def _():
            @pl.loop(0, EL // UE)
            def _(g):
                for i in range(UE):
                    for c in w2load(b, g * UE + i):
                        c.wait()
                for i in range(UE):
                    e = g * UE + i
                    h = jnp.concatenate([X[e * NF + f] for f in range(NF)], axis=1)
                    XIN[e, :, 0:2 * CW] = _dot(h, w2tile(e)).astype(BF)

                @pl.when(b + 1 < NB)
                def _():
                    for i in range(UE):
                        w2start(b + 1, g * UE + i)

            @pl.when(b == 0)
            def _():
                pl.semaphore_wait(ready, 3)

            sb = SS + (b % 3) * 4

            def make(i):
                ACC[YS + (b % 2) * 4 + i] = combine(2 * i + 1)
                d2d(b, i).start()
                ACC[sb + i] = combine(2 * i)

            def total(i, hops):
                d2d(b, i).wait_recv()
                ACC[sb + i] += ACC[b * 4 + i]
                for k in hops:
                    hop1(b, k).start()

            make(3)
            make(2)
            total(3, (1, 3))
            make(1)
            total(2, (0,))
            make(0)
            total(1, (2,))
            total(0, ())
            for i in range(4):
                d2d(b, i).wait_send()

        c = b - 1

        @pl.when((c >= 0) & (c < NB))
        def _():
            sc = SS + (c % 3) * 4
            for k, i, half in ((1, 1, slice(0, CW)), (3, 2, slice(CW, 2 * CW))):
                hop1(c, k).wait_recv()
                ACC[TT + c % 2, :, half] = ACC[sc + i, :, half] + ACC[R1 + c * 2 + 1, :, half]
                hop2(c, (k - 1) // 2).start()
            for k in range(4):
                hop1(c, k).wait_send()

        f = b - 2

        @pl.when(f >= 0)
        def _():
            sf = SS + (f % 3) * 4
            hop1(f, 0).wait_recv()
            hop1(f, 2).wait_recv()
            for k, half in ((0, slice(0, CW)), (1, slice(CW, 2 * CW))):
                hop2(f, k).wait_recv()
                X[OUT + f, :, half] = (ACC[sf, :, half] + ACC[R1 + f * 2, :, half] + ACC[R2 + f, :, half]).astype(BF)
                hop2(f, k).wait_send()
            store(f).start()

    @pl.loop(0, NB)
    def _(b):
        store(b).wait()


def solution(mesh):
    tok = P(('data', 'outer', 'expert'), None)
    wsp = P(('outer', 'expert'), None, None)

    def local(x, wr, idx, w1, w3, w2):
        T, D = x.shape
        E = wr.shape[1]
        EL, _, FF = w1.shape
        K = idx.shape[1]
        C = 2 * T * K // E
        S = EL * C
        NU = D // U
        NB = D // (2 * CW)
        NF = FF // U
        any_ = pl.BlockSpec(memory_space=pl.ANY)
        dma = pltpu.SemaphoreType.DMA
        return pl.pallas_call(
            kernel,
            out_shape=jax.ShapeDtypeStruct((T, D), BF),
            in_specs=[any_] * 6,
            out_specs=any_,
            scratch_shapes=[
                pltpu.VMEM((NU * 8, T, U), BF),
                pltpu.VMEM((K, T), jnp.int32),
                pltpu.VMEM((E, T), F32),
                pltpu.VMEM((8 * EL, T), F32),
                pltpu.VMEM((8 * EL, T), F32),
                pltpu.VMEM((8, S, T), BF),
                pltpu.VMEM((24, T, S), BF),
                pltpu.VMEM((EL, 8 * C, 2 * U), BF),
                pltpu.VMEM((EL * 2 * NF, 8 * C, U), F32),
                pltpu.VMEM((NWT, 2, 2 * U, FF), BF),
                dma((2 * NU + 1,)), dma((NWT, 2)), dma((EL, 2)),
                dma((8, NU)), dma((8, NU)), dma((8,)), dma((8,)),
                dma((NB, 4)), dma((NB, 4)), dma((NB, 4)), dma((NB, 4)), dma((NB, 2)), dma((NB, 2)), dma((NB,)),
                pltpu.SemaphoreType.REGULAR,
            ],
            compiler_params=pltpu.CompilerParams(collective_id=0, has_side_effects=True, vmem_limit_bytes=67043328),
        )(x, wr, idx.T, w1, w3, w2)

    return jax.shard_map(local, mesh=mesh, in_specs=(tok, P(None, None), tok, wsp, wsp, wsp), out_specs=tok, check_vma=False)
```

```python
import functools

import jax
import jax.numpy as jnp
from jax import lax
from jax.experimental import pallas as pl
from jax.experimental.pallas import tpu as pltpu
from jax.sharding import PartitionSpec as P

MESH = pl.DeviceIdType.MESH
BF = jnp.bfloat16
F32 = jnp.float32
U = 256
CW = 128
UA = 8
UE = 4
NWT = 24


def _dot(a, b):
    return jnp.dot(a, b, preferred_element_type=F32)


def kernel(x_hbm, wr_hbm, idx_hbm, w1_hbm, w3_hbm, w2_hbm, out_hbm,
           X, IDX, ET, EX, POS, HT, W, XIN, ACC, WT,
           xsem, wtsem, w2sem, dsend, drecv, esend, erecv,
           d2s, d2r, p1s, p1r, p2s, p2r, osem, ready):
    T, D = x_hbm.shape
    E = wr_hbm.shape[1]
    EL, _, FF = w1_hbm.shape
    K = idx_hbm.shape[0]
    C = 2 * T * K // E
    S = EL * C
    NU = D // U
    NG = EL // UA
    NB = D // (2 * CW)
    NF = FF // U

    dd = lax.axis_index("data")
    oy = lax.axis_index("outer")
    jx = lax.axis_index("expert")
    cx = jx // 2
    cc = jx - 2 * cx
    nx = lax.axis_size("expert")

    def dev(r):
        ry, rx, rc = r // 4, (r // 2) % 2, r % 2
        y = 1 - oy if ry else oy
        x = 1 - cx if rx else cx
        c = 1 - cc if rc else cc
        return y, x * 2 + c

    def did(r):
        y, j = dev(r)
        return (dd, y, j)

    def pos_of(r):
        y, j = dev(r)
        return y * nx + j

    def xload(u):
        return pltpu.make_async_copy(x_hbm.at[:, pl.ds(u * U, U)], X.at[u * 8], xsem.at[u])

    def wrload(u):
        return pltpu.make_async_copy(wr_hbm.at[pl.ds(u * U, U)], XIN.at[u, :, 0:E], xsem.at[NU + u])

    idxload = pltpu.make_async_copy(idx_hbm, IDX, xsem.at[2 * NU])

    def wtload(k, i, m):
        src = w1_hbm if m == 0 else w3_hbm
        rows = pl.ds(pl.multiple_of((k // NG) * U, U), U)
        s = (k % 3) * UA + i
        return pltpu.make_async_copy(src.at[(k % NG) * UA + i, rows, :], WT.at[s, m], wtsem.at[s, m])

    def wtstart(k):
        for i in range(UA):
            for m in range(2):
                wtload(k, i, m).start()

    def wtwait(k):
        for i in range(UA):
            for m in range(2):
                wtload(k, i, m).wait()

    def w2place(b, e):
        return UA * (1 + b % 2) + e // 2, e % 2

    def w2load(b, e):
        cols = pl.ds(pl.multiple_of(b * 2 * CW, 2 * CW), 2 * CW)
        s, m = w2place(b, e)
        return [pltpu.make_async_copy(w2_hbm.at[e, pl.ds(f * U, U), cols], WT.at[s, m, :, f * U:(f + 1) * U],
                                      w2sem.at[b % 2, e, f]) for f in range(NF)]

    def w2start(b, e):
        for c in w2load(b, e):
            c.start()

    def w2tile(b, e):
        s, m = w2place(b, e)
        return jnp.concatenate([WT[s, m, :, f * U:(f + 1) * U] for f in range(NF)], axis=0)

    H = T // 2

    def blk(u, r, half=None):
        b = u * 8 + r
        if half is None:
            return X.at[b]
        return X.at[b, pl.ds(half * H, H)]

    def disp(k, u):
        src, dst, to = [
            (blk(u, 0), blk(u, 2), 2), (blk(u, 0), blk(u, 4), 4), (blk(u, 0), blk(u, 1), 1),
            (blk(u, 2, 0), blk(u, 6, 0), 4), (blk(u, 4, 1), blk(u, 6, 1), 2),
            (blk(u, 2), blk(u, 3), 1), (blk(u, 4), blk(u, 5), 1), (blk(u, 6), blk(u, 7), 1),
        ][k]
        return pltpu.make_async_remote_copy(src_ref=src, dst_ref=dst, send_sem=dsend.at[k, u], recv_sem=drecv.at[k, u],
                                            device_id=did(to), device_id_type=MESH)

    def own(u):
        for k in (0, 1, 2):
            disp(k, u).start()

    def fwd(u):
        disp(0, u).wait_recv()
        disp(1, u).wait_recv()
        for k in (3, 4, 5, 6):
            disp(k, u).start()

    def diag(u):
        disp(3, u).wait_recv()
        disp(4, u).wait_recv()
        disp(7, u).start()

    def arrived(u):
        for k in (2, 5, 6, 7):
            disp(k, u).wait_recv()

    def sent(u):
        for k in range(8):
            disp(k, u).wait_send()

    def ecopy(r):
        rows = pl.ds(pl.multiple_of(pos_of(r) * EL, EL), EL)
        return pltpu.make_async_remote_copy(src_ref=ET.at[rows], dst_ref=EX.at[pl.ds(r * EL, EL)],
                                            send_sem=esend.at[r], recv_sem=erecv.at[r],
                                            device_id=did(r), device_id_type=MESH)

    for u in range(NU):
        xload(u).start()
    for u in range(NU):
        wrload(u).start()
    idxload.start()
    for k in range(3):
        wtstart(k)

    barrier = pltpu.get_barrier_semaphore()
    for r in range(1, 8):
        pl.semaphore_signal(barrier, inc=1, device_id=did(r), device_id_type=MESH)
    xload(0).wait()
    pl.semaphore_wait(barrier, 7)
    own(0)

    for u in range(1, NU):
        xload(u).wait()
    for u in range(NU):
        wrload(u).wait()
    idxload.wait()
    logits = _dot(X[0], XIN[0, :, 0:E])
    for u in range(1, NU):
        logits = logits + _dot(X[u * 8], XIN[u, :, 0:E])
    lane = lax.broadcasted_iota(jnp.int32, (T, E), 1)
    ids = jnp.transpose(IDX[...].astype(F32)).astype(jnp.int32)
    chosen = lane == ids[:, 0:1]
    for j in range(1, K):
        chosen = chosen | (lane == ids[:, j:j + 1])
    top = jnp.max(jnp.where(chosen, logits, -jnp.inf), axis=1, keepdims=True)
    ex = jnp.where(chosen, jnp.exp(jnp.where(chosen, logits - top, 0.0)), 0.0)
    g = ex / jnp.sum(ex, axis=1, keepdims=True)
    ET[...] = jnp.transpose(jnp.where(chosen, g, -1.0))
    for r in range(1, 8):
        ecopy(r).start()
    fwd(0)
    own(1)
    own(2)

    mine = pl.ds(pl.multiple_of(pos_of(0) * EL, EL), EL)
    EX[0:EL] = ET[mine]
    for r in range(1, 8):
        ecopy(r).wait_recv()

    ev = EX[...]
    sel = ev >= 0.0
    before = lax.broadcasted_iota(jnp.int32, (T, T), 0) < lax.broadcasted_iota(jnp.int32, (T, T), 1)
    cnt = _dot(sel.astype(F32).astype(BF), before.astype(F32).astype(BF))
    pos = jnp.where(sel, cnt, -1.0)
    POS[...] = pos

    @pl.loop(0, 8)
    def _(r):
        p = POS[pl.ds(pl.multiple_of(r * EL, EL), EL)]
        slot = lax.broadcasted_iota(jnp.int32, (C, T), 0).astype(F32)
        for e in range(EL):
            HT[r, e * C:(e + 1) * C, :] = jnp.where(jnp.broadcast_to(p[e:e + 1], (C, T)) == slot, 1.0, 0.0).astype(BF)

    ge = jnp.maximum(ev, 0.0)
    post = jnp.transpose(pos).astype(BF)
    gt = jnp.transpose(ge)
    hi = gt.astype(BF)
    rest = gt - hi.astype(F32)
    mid = rest.astype(BF)
    lo = (rest - mid.astype(F32)).astype(BF)

    def weigh(r0):
        @pl.loop(r0, r0 + 4)
        def _(r):
            spread = jnp.where(lax.broadcasted_iota(jnp.int32, (8 * EL, S), 0)
                               == r * EL + lax.broadcasted_iota(jnp.int32, (8 * EL, S), 1) // C, 1.0, 0.0).astype(BF)
            slot = (lax.broadcasted_iota(jnp.int32, (T, S), 1) % C).astype(F32)
            hit = _dot(post, spread) == slot
            for k, part in enumerate((hi, mid, lo)):
                W[k * 8 + r] = jnp.where(hit, _dot(part, spread), 0.0).astype(BF)

    def gather(u):
        @pl.loop(0, 2)
        def _(g):
            for i in range(4):
                r = g * 4 + i
                rows = pl.ds(pl.multiple_of(r * C, C), C)
                XIN[:, rows, :] = _dot(HT[r], X[u * 8 + r]).astype(BF).reshape(EL, C, U)

    def experts(k, put):
        wtwait(k)
        for i in range(UA):
            e, s = (k % NG) * UA + i, (k % 3) * UA + i
            xe = XIN[e]
            for f in range(NF):
                put(e, f, _dot(xe, WT[s, 0, :, f * U:(f + 1) * U]), _dot(xe, WT[s, 1, :, f * U:(f + 1) * U]))

    def first(e, f, a, b):
        ACC[e * 2 * NF + f] = a
        ACC[(e * 2 + 1) * NF + f] = b

    def middle(e, f, a, b):
        ACC[e * 2 * NF + f] += a
        ACC[(e * 2 + 1) * NF + f] += b

    def last(e, f, a, b):
        a = ACC[e * 2 * NF + f] + a
        b = ACC[(e * 2 + 1) * NF + f] + b
        X[e * NF + f] = (jax.nn.silu(a) * b).astype(BF)

    weigh(0)
    fwd(1)
    own(3)
    diag(0)
    arrived(0)
    gather(0)

    @pl.loop(0, NG)
    def _(g):
        experts(g, first)
        wtstart(g + 3)

        @pl.when(g == 0)
        def _():
            fwd(2)
            own(4)

    diag(1)
    weigh(4)

    @pl.loop(1, NU - 1)
    def _(u):
        arrived(u)
        gather(u)

        @pl.loop(0, NG)
        def _(g):
            k = u * NG + g
            experts(k, middle)

            @pl.when(k + 3 < NU * NG)
            def _():
                wtstart(k + 3)

            @pl.when(k + 3 == NU * NG)
            def _():
                for e in range(EL):
                    w2start(0, e)

            @pl.when(g == 0)
            def _():
                diag(u + 1)

                @pl.when(u + 2 < NU)
                def _():
                    fwd(u + 2)

                @pl.when(u + 4 < NU)
                def _():
                    own(u + 4)

    arrived(NU - 1)
    gather(NU - 1)

    @pl.loop(0, NU)
    def _(u):
        sent(u)

    for r in range(1, 8):
        ecopy(r).wait_send()

    @pl.loop(0, NG)
    def _(g):
        experts((NU - 1) * NG + g, last)

        @pl.when(g == 0)
        def _():
            for e in range(EL):
                w2start(1, e)

    for r in (1, 2, 4):
        pl.semaphore_signal(ready, inc=1, device_id=did(r), device_id_type=MESH)

    R1 = 4 * NB
    R2 = R1 + 2 * NB
    YS = R2 + NB
    SS = YS + 8
    TT = SS + 16
    OUT = EL * NF

    def store(b):
        cols = pl.ds(pl.multiple_of(b * 2 * CW, 2 * CW), 2 * CW)
        return pltpu.make_async_copy(X.at[OUT + b], out_hbm.at[:, cols], osem.at[b])

    A = pl.ds(0, CW)
    B = pl.ds(CW, CW)

    def d2d(b, i):
        return pltpu.make_async_remote_copy(
            src_ref=ACC.at[YS + (b % 2) * 4 + i], dst_ref=ACC.at[b * 4 + i],
            send_sem=d2s.at[b, i], recv_sem=d2r.at[b, i], device_id=did(1), device_id_type=MESH)

    def hop1(b, k):
        src, dst, half, to = [(2, 0, A, 4), (3, 1, A, 4), (1, 0, B, 2), (3, 1, B, 2)][k]
        return pltpu.make_async_remote_copy(
            src_ref=ACC.at[SS + (b % 4) * 4 + src, :, half], dst_ref=ACC.at[R1 + b * 2 + dst, :, half],
            send_sem=p1s.at[b, k], recv_sem=p1r.at[b, k], device_id=did(to), device_id_type=MESH)

    def hop2(b, k):
        half, to = [(A, 2), (B, 4)][k]
        return pltpu.make_async_remote_copy(
            src_ref=ACC.at[TT + b % 4, :, half], dst_ref=ACC.at[R2 + b, :, half],
            send_sem=p2s.at[b, k], recv_sem=p2r.at[b, k], device_id=did(to), device_id_type=MESH)

    def combine(r):
        rows = slice(r * C, (r + 1) * C)
        o = XIN[:, rows, :].reshape(S, 2 * CW)
        return _dot(W[r], o) + _dot(W[8 + r], o) + _dot(W[16 + r], o)

    @pl.loop(0, NB + 3)
    def _(b):
        @pl.when(b < NB)
        def _():
            @pl.loop(0, EL // UE)
            def _(g):
                for i in range(UE):
                    for c in w2load(b, g * UE + i):
                        c.wait()
                for i in range(UE):
                    e = g * UE + i
                    h = jnp.concatenate([X[e * NF + f] for f in range(NF)], axis=1)
                    XIN[e] = _dot(h, w2tile(b, e)).astype(BF)

                @pl.when(b + 2 < NB)
                def _():
                    for i in range(UE):
                        w2start(b + 2, g * UE + i)

            @pl.when(b == 0)
            def _():
                pl.semaphore_wait(ready, 3)

            sb = SS + (b % 4) * 4

            def make(i):
                ACC[YS + (b % 2) * 4 + i] = combine(2 * i + 1)
                d2d(b, i).start()
                ACC[sb + i] = combine(2 * i)

            def total(i, hops):
                d2d(b, i).wait_recv()
                ACC[sb + i] += ACC[b * 4 + i]
                for k in hops:
                    hop1(b, k).start()

            make(3)
            make(2)
            total(3, (1, 3))
            make(1)
            total(2, (0,))
            make(0)
            total(1, (2,))
            total(0, ())
            for i in range(4):
                d2d(b, i).wait_send()

        c = b - 1

        @pl.when((c >= 0) & (c < NB))
        def _():
            sc = SS + (c % 4) * 4
            for k, i, half in ((1, 1, slice(0, CW)), (3, 2, slice(CW, 2 * CW))):
                hop1(c, k).wait_recv()
                ACC[TT + c % 4, :, half] = ACC[sc + i, :, half] + ACC[R1 + c * 2 + 1, :, half]
                hop2(c, (k - 1) // 2).start()

        f = b - 3

        @pl.when(f >= 0)
        def _():
            sf = SS + (f % 4) * 4
            for k in range(4):
                hop1(f, k).wait_send()
            hop1(f, 0).wait_recv()
            hop1(f, 2).wait_recv()
            for k, half in ((0, slice(0, CW)), (1, slice(CW, 2 * CW))):
                hop2(f, k).wait_recv()
                X[OUT + f, :, half] = (ACC[sf, :, half] + ACC[R1 + f * 2, :, half] + ACC[R2 + f, :, half]).astype(BF)
                hop2(f, k).wait_send()
            store(f).start()

    @pl.loop(0, NB)
    def _(b):
        store(b).wait()


def solution(mesh):
    tok = P(('data', 'outer', 'expert'), None)
    wsp = P(('outer', 'expert'), None, None)

    def local(x, wr, idx, w1, w3, w2):
        T, D = x.shape
        E = wr.shape[1]
        EL, _, FF = w1.shape
        K = idx.shape[1]
        C = 2 * T * K // E
        S = EL * C
        NU = D // U
        NB = D // (2 * CW)
        NF = FF // U
        any_ = pl.BlockSpec(memory_space=pl.ANY)
        dma = pltpu.SemaphoreType.DMA
        return pl.pallas_call(
            kernel,
            out_shape=jax.ShapeDtypeStruct((T, D), BF),
            in_specs=[any_] * 6,
            out_specs=any_,
            scratch_shapes=[
                pltpu.VMEM((NU * 8, T, U), BF),
                pltpu.VMEM((K, T), jnp.int32),
                pltpu.VMEM((E, T), F32),
                pltpu.VMEM((8 * EL, T), F32),
                pltpu.VMEM((8 * EL, T), F32),
                pltpu.VMEM((8, S, T), BF),
                pltpu.VMEM((24, T, S), BF),
                pltpu.VMEM((EL, 8 * C, U), BF),
                pltpu.VMEM((EL * 2 * NF, 8 * C, U), F32),
                pltpu.VMEM((NWT, 2, U, FF), BF),
                dma((2 * NU + 1,)), dma((NWT, 2)), dma((2, EL, NF)),
                dma((8, NU)), dma((8, NU)), dma((8,)), dma((8,)),
                dma((NB, 4)), dma((NB, 4)), dma((NB, 4)), dma((NB, 4)), dma((NB, 2)), dma((NB, 2)), dma((NB,)),
                pltpu.SemaphoreType.REGULAR,
            ],
            compiler_params=pltpu.CompilerParams(collective_id=0, has_side_effects=True, vmem_limit_bytes=67043328),
        )(x, wr, idx.T, w1, w3, w2)

    return jax.shard_map(local, mesh=mesh, in_specs=(tok, P(None, None), tok, wsp, wsp, wsp), out_specs=tok, check_vma=False)
```

```python
import functools

import jax
import jax.numpy as jnp
from jax import lax
from jax.experimental import pallas as pl
from jax.experimental.pallas import tpu as pltpu
from jax.sharding import PartitionSpec as P

MESH = pl.DeviceIdType.MESH
BF = jnp.bfloat16
F32 = jnp.float32
U = 256
CW = 128
NWT = 12
UE = 4


def _dot(a, b):
    return jnp.dot(a, b, preferred_element_type=F32)


def kernel(x_hbm, wr_hbm, idx_hbm, w1_hbm, w3_hbm, w2_hbm, out_hbm,
           X, IDX, ET, EX, POS, HT, W, XIN, ACC, WT,
           xsem, wtsem, w2sem, dsend, drecv, esend, erecv,
           d2s, d2r, p1s, p1r, p2s, p2r, osem, ready):
    T, D = x_hbm.shape
    E = wr_hbm.shape[1]
    EL, _, FF = w1_hbm.shape
    K = idx_hbm.shape[0]
    C = 2 * T * K // E
    S = EL * C
    NU = D // U
    NQ = NU // 2
    NB = D // (2 * CW)
    NF = FF // U

    dd = lax.axis_index("data")
    oy = lax.axis_index("outer")
    jx = lax.axis_index("expert")
    cx = jx // 2
    cc = jx - 2 * cx
    nx = lax.axis_size("expert")

    def dev(r):
        ry, rx, rc = r // 4, (r // 2) % 2, r % 2
        y = 1 - oy if ry else oy
        x = 1 - cx if rx else cx
        c = 1 - cc if rc else cc
        return y, x * 2 + c

    def did(r):
        y, j = dev(r)
        return (dd, y, j)

    def pos_of(r):
        y, j = dev(r)
        return y * nx + j

    def xload(u):
        return pltpu.make_async_copy(x_hbm.at[:, pl.ds(u * U, U)], X.at[u * 8], xsem.at[u])

    def wrload(u):
        return pltpu.make_async_copy(wr_hbm.at[pl.ds(u * U, U)], XIN.at[u, :, 0:E], xsem.at[NU + u])

    idxload = pltpu.make_async_copy(idx_hbm, IDX, xsem.at[2 * NU])

    def wtload(n, m):
        q, e, s = n // EL, n % EL, n % NWT
        src = w1_hbm if m == 0 else w3_hbm
        rows = pl.ds(pl.multiple_of(q * 2 * U, 2 * U), 2 * U)
        return pltpu.make_async_copy(src.at[e, rows, :], WT.at[s, m], wtsem.at[s, m])

    R = 2 * U

    def w2load(b, e):
        cols = pl.ds(pl.multiple_of(b * 2 * CW, 2 * CW), 2 * CW)
        s, m = NWT - EL // 2 + e // 2, e % 2
        return (
            pltpu.make_async_copy(w2_hbm.at[e, 0:R, cols], WT.at[s, m, :, 0:2 * CW], w2sem.at[e, 0]),
            pltpu.make_async_copy(w2_hbm.at[e, R:FF, cols], WT.at[s, m, 0:FF - R, 2 * CW:4 * CW], w2sem.at[e, 1]))

    def w2start(b, e):
        for c in w2load(b, e):
            c.start()

    def w2tile(e):
        s, m = NWT - EL // 2 + e // 2, e % 2
        return jnp.concatenate([WT[s, m, :, 0:2 * CW], WT[s, m, 0:FF - R, 2 * CW:4 * CW]], axis=0)

    H = T // 2

    def blk(u, r, half=None):
        b = u * 8 + r
        if half is None:
            return X.at[b]
        return X.at[b, pl.ds(half * H, H)]

    def disp(k, u):
        src, dst, to = [
            (blk(u, 0), blk(u, 2), 2), (blk(u, 0), blk(u, 4), 4), (blk(u, 0), blk(u, 1), 1),
            (blk(u, 2, 0), blk(u, 6, 0), 4), (blk(u, 4, 1), blk(u, 6, 1), 2),
            (blk(u, 2), blk(u, 3), 1), (blk(u, 4), blk(u, 5), 1), (blk(u, 6), blk(u, 7), 1),
        ][k]
        return pltpu.make_async_remote_copy(src_ref=src, dst_ref=dst, send_sem=dsend.at[k, u], recv_sem=drecv.at[k, u],
                                            device_id=did(to), device_id_type=MESH)

    def own(u):
        for k in (0, 1, 2):
            disp(k, u).start()

    def fwd(u):
        disp(0, u).wait_recv()
        disp(1, u).wait_recv()
        for k in (3, 4, 5, 6):
            disp(k, u).start()

    def diag(u):
        disp(3, u).wait_recv()
        disp(4, u).wait_recv()
        disp(7, u).start()

    def arrived(u):
        for k in (2, 5, 6, 7):
            disp(k, u).wait_recv()

    def sent(u):
        for k in range(8):
            disp(k, u).wait_send()

    def ecopy(r):
        rows = pl.ds(pl.multiple_of(pos_of(r) * EL, EL), EL)
        return pltpu.make_async_remote_copy(src_ref=ET.at[rows], dst_ref=EX.at[pl.ds(r * EL, EL)],
                                            send_sem=esend.at[r], recv_sem=erecv.at[r],
                                            device_id=did(r), device_id_type=MESH)

    for u in range(NU):
        xload(u).start()
    for u in range(NU):
        wrload(u).start()
    idxload.start()
    for n in range(NWT):
        wtload(n, 0).start()
        wtload(n, 1).start()

    barrier = pltpu.get_barrier_semaphore()
    for r in range(1, 8):
        pl.semaphore_signal(barrier, inc=1, device_id=did(r), device_id_type=MESH)
    xload(0).wait()
    pl.semaphore_wait(barrier, 7)
    own(0)

    for u in range(1, NU):
        xload(u).wait()
    for u in range(NU):
        wrload(u).wait()
    idxload.wait()
    logits = _dot(X[0], XIN[0, :, 0:E])
    for u in range(1, NU):
        logits = logits + _dot(X[u * 8], XIN[u, :, 0:E])
    lane = lax.broadcasted_iota(jnp.int32, (T, E), 1)
    ids = jnp.transpose(IDX[...].astype(F32)).astype(jnp.int32)
    chosen = lane == ids[:, 0:1]
    for j in range(1, K):
        chosen = chosen | (lane == ids[:, j:j + 1])
    top = jnp.max(jnp.where(chosen, logits, -jnp.inf), axis=1, keepdims=True)
    ex = jnp.where(chosen, jnp.exp(jnp.where(chosen, logits - top, 0.0)), 0.0)
    g = ex / jnp.sum(ex, axis=1, keepdims=True)
    ET[...] = jnp.transpose(jnp.where(chosen, g, -1.0))
    for r in range(1, 8):
        ecopy(r).start()
    own(1)

    @pl.loop(0, ACC.shape[0])
    def _(i):
        ACC[i] = jnp.zeros((U, U), F32)

    fwd(0)

    mine = pl.ds(pl.multiple_of(pos_of(0) * EL, EL), EL)
    EX[0:EL] = ET[mine]
    for r in range(1, 8):
        ecopy(r).wait_recv()

    ev = EX[...]
    sel = ev >= 0.0
    before = lax.broadcasted_iota(jnp.int32, (T, T), 0) < lax.broadcasted_iota(jnp.int32, (T, T), 1)
    cnt = _dot(sel.astype(F32).astype(BF), before.astype(F32).astype(BF))
    pos = jnp.where(sel, cnt, -1.0)
    POS[...] = pos

    @pl.loop(0, 8)
    def _(r):
        p = POS[pl.ds(pl.multiple_of(r * EL, EL), EL)]
        slot = lax.broadcasted_iota(jnp.int32, (C, T), 0).astype(F32)
        for e in range(EL):
            HT[r, e * C:(e + 1) * C, :] = jnp.where(jnp.broadcast_to(p[e:e + 1], (C, T)) == slot, 1.0, 0.0).astype(BF)

    ge = jnp.maximum(ev, 0.0)
    post = jnp.transpose(pos).astype(BF)
    gt = jnp.transpose(ge)
    hi = gt.astype(BF)
    rest = gt - hi.astype(F32)
    mid = rest.astype(BF)
    lo = (rest - mid.astype(F32)).astype(BF)

    def weigh(r):
        spread = jnp.where(lax.broadcasted_iota(jnp.int32, (8 * EL, S), 0)
                           == r * EL + lax.broadcasted_iota(jnp.int32, (8 * EL, S), 1) // C, 1.0, 0.0).astype(BF)
        slot = (lax.broadcasted_iota(jnp.int32, (T, S), 1) % C).astype(F32)
        hit = _dot(post, spread) == slot
        for k, part in enumerate((hi, mid, lo)):
            W[k * 8 + r] = jnp.where(hit, _dot(part, spread), 0.0).astype(BF)

    pl.loop(0, 4)(weigh)
    fwd(1)
    own(2)
    own(3)
    pl.loop(4, 8)(weigh)
    diag(0)
    diag(1)
    arrived(0)
    arrived(1)

    def gather(q):
        for r in range(8):
            for s in range(2):
                v = _dot(HT[r], X[(2 * q + s) * 8 + r])
                XIN[:, r * C:(r + 1) * C, s * U:(s + 1) * U] = v.astype(BF).reshape(EL, C, U)

    def tiles(n):
        for i in range(UE):
            for m in range(2):
                wtload(n + i, m).wait()

    @pl.loop(0, NQ - 1)
    def _(q):
        u = 2 * q + 2
        gather(q)
        fwd(u)

        @pl.when(u + 2 < NU)
        def _():
            own(u + 2)


        @pl.loop(0, EL // UE)
        def _(g):
            n = q * EL + g * UE
            tiles(n)
            for i in range(UE):
                e, s = g * UE + i, n % NWT + i
                xe = XIN[e]
                for m in range(2):
                    for f in range(NF):
                        ACC[(e * 2 + m) * NF + f] += _dot(xe, WT[s, m, :, f * U:(f + 1) * U])
            for i in range(UE):
                for m in range(2):
                    wtload(n + NWT + i, m).start()

            @pl.when(g == 1)
            def _():
                diag(u)
                fwd(u + 1)

                @pl.when(u + 3 < NU)
                def _():
                    own(u + 3)

        diag(u + 1)
        arrived(u)
        arrived(u + 1)

    gather(NQ - 1)

    @pl.loop(0, NU)
    def _(u):
        sent(u)

    for r in range(1, 8):
        ecopy(r).wait_send()

    @pl.loop(0, EL // UE)
    def _(g):
        n = (NQ - 1) * EL + g * UE
        tiles(n)
        for i in range(UE):
            e, s = g * UE + i, n % NWT + i
            xe = XIN[e]
            for f in range(NF):
                a = ACC[e * 2 * NF + f] + _dot(xe, WT[s, 0, :, f * U:(f + 1) * U])
                b = ACC[(e * 2 + 1) * NF + f] + _dot(xe, WT[s, 1, :, f * U:(f + 1) * U])
                X[e * NF + f] = (jax.nn.silu(a) * b).astype(BF)

        @pl.when(n + NWT < NQ * EL)
        def _():
            for i in range(UE):
                for m in range(2):
                    wtload(n + NWT + i, m).start()

        @pl.when((g == 1) | (g == 2))
        def _():
            for i in range(2 * UE):
                w2start(0, (g - 1) * 2 * UE + i)

    for r in (1, 2, 4):
        pl.semaphore_signal(ready, inc=1, device_id=did(r), device_id_type=MESH)

    R1 = 4 * NB
    R2 = R1 + 2 * NB
    YS = R2 + NB
    SS = YS + 8
    TT = SS + 16
    OUT = EL * NF

    def store(b):
        cols = pl.ds(pl.multiple_of(b * 2 * CW, 2 * CW), 2 * CW)
        return pltpu.make_async_copy(X.at[OUT + b], out_hbm.at[:, cols], osem.at[b])

    A = pl.ds(0, CW)
    B = pl.ds(CW, CW)

    def d2d(b, i):
        return pltpu.make_async_remote_copy(
            src_ref=ACC.at[YS + (b % 2) * 4 + i], dst_ref=ACC.at[b * 4 + i],
            send_sem=d2s.at[b, i], recv_sem=d2r.at[b, i], device_id=did(1), device_id_type=MESH)

    def hop1(b, k):
        src, dst, half, to = [(2, 0, A, 4), (3, 1, A, 4), (1, 0, B, 2), (3, 1, B, 2)][k]
        return pltpu.make_async_remote_copy(
            src_ref=ACC.at[SS + (b % 4) * 4 + src, :, half], dst_ref=ACC.at[R1 + b * 2 + dst, :, half],
            send_sem=p1s.at[b, k], recv_sem=p1r.at[b, k], device_id=did(to), device_id_type=MESH)

    def hop2(b, k):
        half, to = [(A, 2), (B, 4)][k]
        return pltpu.make_async_remote_copy(
            src_ref=ACC.at[TT + b % 4, :, half], dst_ref=ACC.at[R2 + b, :, half],
            send_sem=p2s.at[b, k], recv_sem=p2r.at[b, k], device_id=did(to), device_id_type=MESH)

    def combine(r):
        rows = slice(r * C, (r + 1) * C)
        o = XIN[:, rows, 0:2 * CW].reshape(S, 2 * CW)
        return _dot(W[r], o) + _dot(W[8 + r], o) + _dot(W[16 + r], o)

    @pl.loop(0, NB + 3)
    def _(b):
        @pl.when(b < NB)
        def _():
            for e in range(EL):
                for c in w2load(b, e):
                    c.wait()
            for e in range(EL):
                h = jnp.concatenate([X[e * NF + f] for f in range(NF)], axis=1)
                XIN[e, :, 0:2 * CW] = _dot(h, w2tile(e)).astype(BF)

            @pl.when(b + 1 < NB)
            def _():
                for e in range(EL):
                    w2start(b + 1, e)

            @pl.when(b == 0)
            def _():
                pl.semaphore_wait(ready, 3)

            sb = SS + (b % 4) * 4

            def make(i):
                ACC[YS + (b % 2) * 4 + i] = combine(2 * i + 1)
                d2d(b, i).start()
                ACC[sb + i] = combine(2 * i)

            def total(i, hops):
                d2d(b, i).wait_recv()
                ACC[sb + i] += ACC[b * 4 + i]
                for k in hops:
                    hop1(b, k).start()

            make(3)
            make(2)
            total(3, (1, 3))
            make(1)
            total(2, (0,))
            make(0)
            total(1, (2,))
            total(0, ())
            for i in range(4):
                d2d(b, i).wait_send()

        c = b - 1

        @pl.when((c >= 0) & (c < NB))
        def _():
            sc = SS + (c % 4) * 4
            for k, i, half in ((1, 1, slice(0, CW)), (3, 2, slice(CW, 2 * CW))):
                hop1(c, k).wait_recv()
                ACC[TT + c % 4, :, half] = ACC[sc + i, :, half] + ACC[R1 + c * 2 + 1, :, half]
                hop2(c, (k - 1) // 2).start()

        f = b - 3

        @pl.when(f >= 0)
        def _():
            sf = SS + (f % 4) * 4
            for k in range(4):
                hop1(f, k).wait_send()
            hop1(f, 0).wait_recv()
            hop1(f, 2).wait_recv()
            for k, half in ((0, slice(0, CW)), (1, slice(CW, 2 * CW))):
                hop2(f, k).wait_recv()
                X[OUT + f, :, half] = (ACC[sf, :, half] + ACC[R1 + f * 2, :, half] + ACC[R2 + f, :, half]).astype(BF)
                hop2(f, k).wait_send()
            store(f).start()

    @pl.loop(0, NB)
    def _(b):
        store(b).wait()


def solution(mesh):
    tok = P(('data', 'outer', 'expert'), None)
    wsp = P(('outer', 'expert'), None, None)

    def local(x, wr, idx, w1, w3, w2):
        T, D = x.shape
        E = wr.shape[1]
        EL, _, FF = w1.shape
        K = idx.shape[1]
        C = 2 * T * K // E
        S = EL * C
        NU = D // U
        NB = D // (2 * CW)
        NF = FF // U
        any_ = pl.BlockSpec(memory_space=pl.ANY)
        dma = pltpu.SemaphoreType.DMA
        return pl.pallas_call(
            kernel,
            out_shape=jax.ShapeDtypeStruct((T, D), BF),
            in_specs=[any_] * 6,
            out_specs=any_,
            scratch_shapes=[
                pltpu.VMEM((NU * 8, T, U), BF),
                pltpu.VMEM((K, T), jnp.int32),
                pltpu.VMEM((E, T), F32),
                pltpu.VMEM((8 * EL, T), F32),
                pltpu.VMEM((8 * EL, T), F32),
                pltpu.VMEM((8, S, T), BF),
                pltpu.VMEM((24, T, S), BF),
                pltpu.VMEM((EL, 8 * C, 2 * U), BF),
                pltpu.VMEM((EL * 2 * NF, 8 * C, U), F32),
                pltpu.VMEM((NWT, 2, 2 * U, FF), BF),
                dma((2 * NU + 1,)), dma((NWT, 2)), dma((EL, 2)),
                dma((8, NU)), dma((8, NU)), dma((8,)), dma((8,)),
                dma((NB, 4)), dma((NB, 4)), dma((NB, 4)), dma((NB, 4)), dma((NB, 2)), dma((NB, 2)), dma((NB,)),
                pltpu.SemaphoreType.REGULAR,
            ],
            compiler_params=pltpu.CompilerParams(collective_id=0, has_side_effects=True, vmem_limit_bytes=67043328),
        )(x, wr, idx.T, w1, w3, w2)

    return jax.shard_map(local, mesh=mesh, in_specs=(tok, P(None, None), tok, wsp, wsp, wsp), out_specs=tok, check_vma=False)
```

```python
import functools

import jax
import jax.numpy as jnp
from jax import lax
from jax.experimental import pallas as pl
from jax.experimental.pallas import tpu as pltpu
from jax.sharding import PartitionSpec as P

MESH = pl.DeviceIdType.MESH
BF = jnp.bfloat16
F32 = jnp.float32
U = 256
CW = 128
NWT = 12
UE = 4


def _dot(a, b):
    return jnp.dot(a, b, preferred_element_type=F32)


def kernel(x_hbm, wr_hbm, idx_hbm, w1_hbm, w3_hbm, w2_hbm, out_hbm,
           X, IDX, ET, EX, POS, HT, W, XIN, ACC, WT,
           xsem, wtsem, w2sem, dsend, drecv, esend, erecv,
           d2s, d2r, p1s, p1r, p2s, p2r, osem, ready):
    T, D = x_hbm.shape
    E = wr_hbm.shape[1]
    EL, _, FF = w1_hbm.shape
    K = idx_hbm.shape[0]
    C = 2 * T * K // E
    S = EL * C
    NU = D // U
    NQ = NU // 2
    NB = D // (2 * CW)
    NF = FF // U

    dd = lax.axis_index("data")
    oy = lax.axis_index("outer")
    jx = lax.axis_index("expert")
    cx = jx // 2
    cc = jx - 2 * cx
    nx = lax.axis_size("expert")

    def dev(r):
        ry, rx, rc = r // 4, (r // 2) % 2, r % 2
        y = 1 - oy if ry else oy
        x = 1 - cx if rx else cx
        c = 1 - cc if rc else cc
        return y, x * 2 + c

    def did(r):
        y, j = dev(r)
        return (dd, y, j)

    def pos_of(r):
        y, j = dev(r)
        return y * nx + j

    def xload(u):
        return pltpu.make_async_copy(x_hbm.at[:, pl.ds(u * U, U)], X.at[u * 8], xsem.at[u])

    def wrload(u):
        return pltpu.make_async_copy(wr_hbm.at[pl.ds(u * U, U)], XIN.at[u, :, 0:E], xsem.at[NU + u])

    idxload = pltpu.make_async_copy(idx_hbm, IDX, xsem.at[2 * NU])

    def wtload(n, m):
        q, e, s = n // EL, n % EL, n % NWT
        src = w1_hbm if m == 0 else w3_hbm
        rows = pl.ds(pl.multiple_of(q * 2 * U, 2 * U), 2 * U)
        return pltpu.make_async_copy(src.at[e, rows, :], WT.at[s, m], wtsem.at[s, m])

    R = 2 * U

    def w2place(b, e):
        p = b % 2
        s, m = NWT - EL // 2 + e // 2, e % 2
        return ((s, m, slice(None), pl.ds(pl.multiple_of(p * 4 * CW, 4 * CW), 2 * CW)),
                (s, m, pl.ds(pl.multiple_of(p * (FF - R), FF - R), FF - R), slice(2 * CW, 4 * CW)))

    def w2load(b, e):
        cols = pl.ds(pl.multiple_of(b * 2 * CW, 2 * CW), 2 * CW)
        top, low = w2place(b, e)
        return (pltpu.make_async_copy(w2_hbm.at[e, 0:R, cols], WT.at[top], w2sem.at[b % 2, e, 0]),
                pltpu.make_async_copy(w2_hbm.at[e, R:FF, cols], WT.at[low], w2sem.at[b % 2, e, 1]))

    def w2start(b, e):
        for c in w2load(b, e):
            c.start()

    def w2tile(b, e):
        top, low = w2place(b, e)
        return jnp.concatenate([WT[top], WT[low]], axis=0)

    H = T // 2

    def blk(u, r, half=None):
        b = u * 8 + r
        if half is None:
            return X.at[b]
        return X.at[b, pl.ds(half * H, H)]

    def disp(k, u):
        src, dst, to = [
            (blk(u, 0), blk(u, 2), 2), (blk(u, 0), blk(u, 4), 4), (blk(u, 0), blk(u, 1), 1),
            (blk(u, 2, 0), blk(u, 6, 0), 4), (blk(u, 4, 1), blk(u, 6, 1), 2),
            (blk(u, 2), blk(u, 3), 1), (blk(u, 4), blk(u, 5), 1), (blk(u, 6), blk(u, 7), 1),
        ][k]
        return pltpu.make_async_remote_copy(src_ref=src, dst_ref=dst, send_sem=dsend.at[k, u], recv_sem=drecv.at[k, u],
                                            device_id=did(to), device_id_type=MESH)

    def own(u):
        for k in (0, 1, 2):
            disp(k, u).start()

    def fwd(u):
        disp(0, u).wait_recv()
        disp(1, u).wait_recv()
        for k in (3, 4, 5, 6):
            disp(k, u).start()

    def diag(u):
        disp(3, u).wait_recv()
        disp(4, u).wait_recv()
        disp(7, u).start()

    def arrived(u):
        for k in (2, 5, 6, 7):
            disp(k, u).wait_recv()

    def sent(u):
        for k in range(8):
            disp(k, u).wait_send()

    def ecopy(r):
        rows = pl.ds(pl.multiple_of(pos_of(r) * EL, EL), EL)
        return pltpu.make_async_remote_copy(src_ref=ET.at[rows], dst_ref=EX.at[pl.ds(r * EL, EL)],
                                            send_sem=esend.at[r], recv_sem=erecv.at[r],
                                            device_id=did(r), device_id_type=MESH)

    for u in range(NU):
        xload(u).start()
    for u in range(NU):
        wrload(u).start()
    idxload.start()

    barrier = pltpu.get_barrier_semaphore()
    for r in range(1, 8):
        pl.semaphore_signal(barrier, inc=1, device_id=did(r), device_id_type=MESH)
    xload(0).wait()
    pl.semaphore_wait(barrier, 7)
    own(0)

    for u in range(1, NU):
        xload(u).wait()
    for u in range(NU):
        wrload(u).wait()
    idxload.wait()
    logits = _dot(X[0], XIN[0, :, 0:E])
    for u in range(1, NU):
        logits = logits + _dot(X[u * 8], XIN[u, :, 0:E])
    lane = lax.broadcasted_iota(jnp.int32, (T, E), 1)
    ids = jnp.transpose(IDX[...].astype(F32)).astype(jnp.int32)
    chosen = lane == ids[:, 0:1]
    for j in range(1, K):
        chosen = chosen | (lane == ids[:, j:j + 1])
    top = jnp.max(jnp.where(chosen, logits, -jnp.inf), axis=1, keepdims=True)
    ex = jnp.where(chosen, jnp.exp(jnp.where(chosen, logits - top, 0.0)), 0.0)
    g = ex / jnp.sum(ex, axis=1, keepdims=True)
    ET[...] = jnp.transpose(jnp.where(chosen, g, -1.0))
    for r in range(1, 8):
        ecopy(r).start()
    own(1)

    @pl.loop(0, ACC.shape[0])
    def _(i):
        ACC[i] = jnp.zeros((U, U), F32)

    fwd(0)
    for n in range(NWT):
        wtload(n, 0).start()
        wtload(n, 1).start()

    mine = pl.ds(pl.multiple_of(pos_of(0) * EL, EL), EL)
    EX[0:EL] = ET[mine]
    for r in range(1, 8):
        ecopy(r).wait_recv()

    ev = EX[...]
    sel = ev >= 0.0
    before = lax.broadcasted_iota(jnp.int32, (T, T), 0) < lax.broadcasted_iota(jnp.int32, (T, T), 1)
    cnt = _dot(sel.astype(F32).astype(BF), before.astype(F32).astype(BF))
    pos = jnp.where(sel, cnt, -1.0)
    POS[...] = pos

    @pl.loop(0, 8)
    def _(r):
        p = POS[pl.ds(pl.multiple_of(r * EL, EL), EL)]
        slot = lax.broadcasted_iota(jnp.int32, (C, T), 0).astype(F32)
        for e in range(EL):
            HT[r, e * C:(e + 1) * C, :] = jnp.where(jnp.broadcast_to(p[e:e + 1], (C, T)) == slot, 1.0, 0.0).astype(BF)

    ge = jnp.maximum(ev, 0.0)
    post = jnp.transpose(pos).astype(BF)
    gt = jnp.transpose(ge)
    hi = gt.astype(BF)
    rest = gt - hi.astype(F32)
    mid = rest.astype(BF)
    lo = (rest - mid.astype(F32)).astype(BF)

    def weigh(r):
        spread = jnp.where(lax.broadcasted_iota(jnp.int32, (8 * EL, S), 0)
                           == r * EL + lax.broadcasted_iota(jnp.int32, (8 * EL, S), 1) // C, 1.0, 0.0).astype(BF)
        slot = (lax.broadcasted_iota(jnp.int32, (T, S), 1) % C).astype(F32)
        hit = _dot(post, spread) == slot
        for k, part in enumerate((hi, mid, lo)):
            W[k * 8 + r] = jnp.where(hit, _dot(part, spread), 0.0).astype(BF)

    pl.loop(0, 4)(weigh)
    fwd(1)
    own(2)
    own(3)
    pl.loop(4, 8)(weigh)
    diag(0)
    diag(1)
    arrived(0)
    arrived(1)

    def gather(q):
        for r in range(8):
            for s in range(2):
                v = _dot(HT[r], X[(2 * q + s) * 8 + r])
                XIN[:, r * C:(r + 1) * C, s * U:(s + 1) * U] = v.astype(BF).reshape(EL, C, U)

    def tiles(n):
        for i in range(UE):
            for m in range(2):
                wtload(n + i, m).wait()

    @pl.loop(0, NQ - 1)
    def _(q):
        u = 2 * q + 2
        gather(q)
        fwd(u)

        @pl.when(u + 2 < NU)
        def _():
            own(u + 2)


        @pl.loop(0, EL // UE)
        def _(g):
            n = q * EL + g * UE
            tiles(n)
            for i in range(UE):
                e, s = g * UE + i, n % NWT + i
                xe = XIN[e]
                for m in range(2):
                    for f in range(NF):
                        ACC[(e * 2 + m) * NF + f] += _dot(xe, WT[s, m, :, f * U:(f + 1) * U])
            @pl.when(g == 1)
            def _():
                diag(u)
                fwd(u + 1)

                @pl.when(u + 3 < NU)
                def _():
                    own(u + 3)

            for i in range(UE):
                for m in range(2):
                    wtload(n + NWT + i, m).start()

        diag(u + 1)
        arrived(u)
        arrived(u + 1)

    gather(NQ - 1)

    @pl.loop(0, NU)
    def _(u):
        sent(u)

    for r in range(1, 8):
        ecopy(r).wait_send()

    @pl.loop(0, EL // UE)
    def _(g):
        n = (NQ - 1) * EL + g * UE
        tiles(n)
        for i in range(UE):
            e, s = g * UE + i, n % NWT + i
            xe = XIN[e]
            for f in range(NF):
                a = ACC[e * 2 * NF + f] + _dot(xe, WT[s, 0, :, f * U:(f + 1) * U])
                b = ACC[(e * 2 + 1) * NF + f] + _dot(xe, WT[s, 1, :, f * U:(f + 1) * U])
                X[e * NF + f] = (jax.nn.silu(a) * b).astype(BF)

        @pl.when(n + NWT < NQ * EL)
        def _():
            for i in range(UE):
                for m in range(2):
                    wtload(n + NWT + i, m).start()

        @pl.when((g == 1) | (g == 2))
        def _():
            for i in range(2 * UE):
                w2start(0, (g - 1) * 2 * UE + i)
                w2start(1, (g - 1) * 2 * UE + i)

    for r in (1, 2, 4):
        pl.semaphore_signal(ready, inc=1, device_id=did(r), device_id_type=MESH)

    R1 = 4 * NB
    R2 = R1 + 2 * NB
    YS = R2 + NB
    SS = YS + 8
    TT = SS + 16
    OUT = EL * NF

    def store(b):
        cols = pl.ds(pl.multiple_of(b * 2 * CW, 2 * CW), 2 * CW)
        return pltpu.make_async_copy(X.at[OUT + b], out_hbm.at[:, cols], osem.at[b])

    A = pl.ds(0, CW)
    B = pl.ds(CW, CW)

    def d2d(b, i):
        return pltpu.make_async_remote_copy(
            src_ref=ACC.at[YS + (b % 2) * 4 + i], dst_ref=ACC.at[b * 4 + i],
            send_sem=d2s.at[b, i], recv_sem=d2r.at[b, i], device_id=did(1), device_id_type=MESH)

    def hop1(b, k):
        src, dst, half, to = [(2, 0, A, 4), (3, 1, A, 4), (1, 0, B, 2), (3, 1, B, 2)][k]
        return pltpu.make_async_remote_copy(
            src_ref=ACC.at[SS + (b % 4) * 4 + src, :, half], dst_ref=ACC.at[R1 + b * 2 + dst, :, half],
            send_sem=p1s.at[b, k], recv_sem=p1r.at[b, k], device_id=did(to), device_id_type=MESH)

    def hop2(b, k):
        half, to = [(A, 2), (B, 4)][k]
        return pltpu.make_async_remote_copy(
            src_ref=ACC.at[TT + b % 4, :, half], dst_ref=ACC.at[R2 + b, :, half],
            send_sem=p2s.at[b, k], recv_sem=p2r.at[b, k], device_id=did(to), device_id_type=MESH)

    def combine(r):
        rows = slice(r * C, (r + 1) * C)
        o = XIN[:, rows, 0:2 * CW].reshape(S, 2 * CW)
        return _dot(W[r], o) + _dot(W[8 + r], o) + _dot(W[16 + r], o)

    @pl.loop(0, NB + 3)
    def _(b):
        @pl.when(b < NB)
        def _():
            for e in range(EL):
                for c in w2load(b, e):
                    c.wait()
            for e in range(EL):
                h = jnp.concatenate([X[e * NF + f] for f in range(NF)], axis=1)
                XIN[e, :, 0:2 * CW] = _dot(h, w2tile(b, e)).astype(BF)

            @pl.when(b == 0)
            def _():
                pl.semaphore_wait(ready, 3)

            sb = SS + (b % 4) * 4

            def make(i):
                ACC[YS + (b % 2) * 4 + i] = combine(2 * i + 1)
                d2d(b, i).start()
                ACC[sb + i] = combine(2 * i)

            def total(i, hops):
                d2d(b, i).wait_recv()
                ACC[sb + i] += ACC[b * 4 + i]
                for k in hops:
                    hop1(b, k).start()

            make(3)
            make(2)
            total(3, (1, 3))
            make(1)
            total(2, (0,))
            make(0)
            total(1, (2,))
            total(0, ())
            for i in range(4):
                d2d(b, i).wait_send()

            @pl.when(b + 2 < NB)
            def _():
                for e in range(EL):
                    w2start(b + 2, e)

        c = b - 1

        @pl.when((c >= 0) & (c < NB))
        def _():
            sc = SS + (c % 4) * 4
            for k, i, half in ((1, 1, slice(0, CW)), (3, 2, slice(CW, 2 * CW))):
                hop1(c, k).wait_recv()
                ACC[TT + c % 4, :, half] = ACC[sc + i, :, half] + ACC[R1 + c * 2 + 1, :, half]
                hop2(c, (k - 1) // 2).start()

        f = b - 3

        @pl.when(f >= 0)
        def _():
            sf = SS + (f % 4) * 4
            for k in range(4):
                hop1(f, k).wait_send()
            hop1(f, 0).wait_recv()
            hop1(f, 2).wait_recv()
            for k, half in ((0, slice(0, CW)), (1, slice(CW, 2 * CW))):
                hop2(f, k).wait_recv()
                X[OUT + f, :, half] = (ACC[sf, :, half] + ACC[R1 + f * 2, :, half] + ACC[R2 + f, :, half]).astype(BF)
                hop2(f, k).wait_send()
            store(f).start()

    @pl.loop(0, NB)
    def _(b):
        store(b).wait()


def solution(mesh):
    tok = P(('data', 'outer', 'expert'), None)
    wsp = P(('outer', 'expert'), None, None)

    def local(x, wr, idx, w1, w3, w2):
        T, D = x.shape
        E = wr.shape[1]
        EL, _, FF = w1.shape
        K = idx.shape[1]
        C = 2 * T * K // E
        S = EL * C
        NU = D // U
        NB = D // (2 * CW)
        NF = FF // U
        any_ = pl.BlockSpec(memory_space=pl.ANY)
        dma = pltpu.SemaphoreType.DMA
        return pl.pallas_call(
            kernel,
            out_shape=jax.ShapeDtypeStruct((T, D), BF),
            in_specs=[any_] * 6,
            out_specs=any_,
            scratch_shapes=[
                pltpu.VMEM((NU * 8, T, U), BF),
                pltpu.VMEM((K, T), jnp.int32),
                pltpu.VMEM((E, T), F32),
                pltpu.VMEM((8 * EL, T), F32),
                pltpu.VMEM((8 * EL, T), F32),
                pltpu.VMEM((8, S, T), BF),
                pltpu.VMEM((24, T, S), BF),
                pltpu.VMEM((EL, 8 * C, 2 * U), BF),
                pltpu.VMEM((EL * 2 * NF, 8 * C, U), F32),
                pltpu.VMEM((NWT, 2, 2 * U, FF), BF),
                dma((2 * NU + 1,)), dma((NWT, 2)), dma((2, EL, 2)),
                dma((8, NU)), dma((8, NU)), dma((8,)), dma((8,)),
                dma((NB, 4)), dma((NB, 4)), dma((NB, 4)), dma((NB, 4)), dma((NB, 2)), dma((NB, 2)), dma((NB,)),
                pltpu.SemaphoreType.REGULAR,
            ],
            compiler_params=pltpu.CompilerParams(collective_id=0, has_side_effects=True, vmem_limit_bytes=67043328),
        )(x, wr, idx.T, w1, w3, w2)

    return jax.shard_map(local, mesh=mesh, in_specs=(tok, P(None, None), tok, wsp, wsp, wsp), out_specs=tok, check_vma=False)
```

```python
import functools

import jax
import jax.numpy as jnp
from jax import lax
from jax.experimental import pallas as pl
from jax.experimental.pallas import tpu as pltpu
from jax.sharding import PartitionSpec as P

MESH = pl.DeviceIdType.MESH
BF = jnp.bfloat16
F32 = jnp.float32
U = 256
CW = 128
NWT = 12
UE = 4


def _dot(a, b):
    return jnp.dot(a, b, preferred_element_type=F32)


def kernel(x_hbm, wr_hbm, idx_hbm, w1_hbm, w3_hbm, w2_hbm, out_hbm,
           X, IDX, ET, EX, POS, HT, W, XIN, ACC, WT,
           xsem, wtsem, w2sem, dsend, drecv, esend, erecv,
           d2s, d2r, p1s, p1r, p2s, p2r, osem, ready):
    T, D = x_hbm.shape
    E = wr_hbm.shape[1]
    EL, _, FF = w1_hbm.shape
    K = idx_hbm.shape[0]
    C = 2 * T * K // E
    S = EL * C
    NU = D // U
    NQ = NU // 2
    NB = D // (2 * CW)
    NF = FF // U

    dd = lax.axis_index("data")
    oy = lax.axis_index("outer")
    jx = lax.axis_index("expert")
    cx = jx // 2
    cc = jx - 2 * cx
    nx = lax.axis_size("expert")

    def dev(r):
        ry, rx, rc = r // 4, (r // 2) % 2, r % 2
        y = 1 - oy if ry else oy
        x = 1 - cx if rx else cx
        c = 1 - cc if rc else cc
        return y, x * 2 + c

    def did(r):
        y, j = dev(r)
        return (dd, y, j)

    def pos_of(r):
        y, j = dev(r)
        return y * nx + j

    def xload(u):
        return pltpu.make_async_copy(x_hbm.at[:, pl.ds(u * U, U)], X.at[u * 8], xsem.at[u])

    def wrload(u):
        return pltpu.make_async_copy(wr_hbm.at[pl.ds(u * U, U)], XIN.at[u, :, 0:E], xsem.at[NU + u])

    idxload = pltpu.make_async_copy(idx_hbm, IDX, xsem.at[2 * NU])

    def wtload(n, m):
        q, e, s = n // EL, n % EL, n % NWT
        src = w1_hbm if m == 0 else w3_hbm
        rows = pl.ds(pl.multiple_of(q * 2 * U, 2 * U), 2 * U)
        return pltpu.make_async_copy(src.at[e, rows, :], WT.at[s, m], wtsem.at[s, m])

    R = 2 * U

    def w2place(b, e):
        p = b % 2
        s, m = NWT - EL // 2 + e // 2, e % 2
        return ((s, m, slice(None), pl.ds(pl.multiple_of(p * 4 * CW, 4 * CW), 2 * CW)),
                (s, m, pl.ds(pl.multiple_of(p * (FF - R), FF - R), FF - R), slice(2 * CW, 4 * CW)))

    def w2load(b, e):
        cols = pl.ds(pl.multiple_of(b * 2 * CW, 2 * CW), 2 * CW)
        top, low = w2place(b, e)
        return (pltpu.make_async_copy(w2_hbm.at[e, 0:R, cols], WT.at[top], w2sem.at[b % 2, e, 0]),
                pltpu.make_async_copy(w2_hbm.at[e, R:FF, cols], WT.at[low], w2sem.at[b % 2, e, 1]))

    def w2start(b, e):
        for c in w2load(b, e):
            c.start()

    def w2tile(b, e):
        top, low = w2place(b, e)
        return jnp.concatenate([WT[top], WT[low]], axis=0)

    H = T // 2

    def blk(u, r, half=None):
        b = u * 8 + r
        if half is None:
            return X.at[b]
        return X.at[b, pl.ds(half * H, H)]

    def disp(k, u):
        src, dst, to = [
            (blk(u, 0), blk(u, 2), 2), (blk(u, 0), blk(u, 4), 4), (blk(u, 0), blk(u, 1), 1),
            (blk(u, 2, 0), blk(u, 6, 0), 4), (blk(u, 4, 1), blk(u, 6, 1), 2),
            (blk(u, 2), blk(u, 3), 1), (blk(u, 4), blk(u, 5), 1), (blk(u, 6), blk(u, 7), 1),
        ][k]
        return pltpu.make_async_remote_copy(src_ref=src, dst_ref=dst, send_sem=dsend.at[k, u], recv_sem=drecv.at[k, u],
                                            device_id=did(to), device_id_type=MESH)

    def own(u):
        for k in (0, 1, 2):
            disp(k, u).start()

    def fwd(u):
        disp(0, u).wait_recv()
        disp(1, u).wait_recv()
        for k in (3, 4, 5, 6):
            disp(k, u).start()

    def diag(u):
        disp(3, u).wait_recv()
        disp(4, u).wait_recv()
        disp(7, u).start()

    def arrived(u):
        for k in (2, 5, 6, 7):
            disp(k, u).wait_recv()

    def sent(u):
        for k in range(8):
            disp(k, u).wait_send()

    def ecopy(r):
        rows = pl.ds(pl.multiple_of(pos_of(r) * EL, EL), EL)
        return pltpu.make_async_remote_copy(src_ref=ET.at[rows], dst_ref=EX.at[pl.ds(r * EL, EL)],
                                            send_sem=esend.at[r], recv_sem=erecv.at[r],
                                            device_id=did(r), device_id_type=MESH)

    for u in range(NU):
        xload(u).start()
    for u in range(NU):
        wrload(u).start()
    idxload.start()

    barrier = pltpu.get_barrier_semaphore()
    for r in range(1, 8):
        pl.semaphore_signal(barrier, inc=1, device_id=did(r), device_id_type=MESH)
    xload(0).wait()
    pl.semaphore_wait(barrier, 7)
    own(0)

    for u in range(1, NU):
        xload(u).wait()
    for u in range(NU):
        wrload(u).wait()
    idxload.wait()
    logits = _dot(X[0], XIN[0, :, 0:E])
    for u in range(1, NU):
        logits = logits + _dot(X[u * 8], XIN[u, :, 0:E])
    lane = lax.broadcasted_iota(jnp.int32, (T, E), 1)
    ids = jnp.transpose(IDX[...].astype(F32)).astype(jnp.int32)
    chosen = lane == ids[:, 0:1]
    for j in range(1, K):
        chosen = chosen | (lane == ids[:, j:j + 1])
    top = jnp.max(jnp.where(chosen, logits, -jnp.inf), axis=1, keepdims=True)
    ex = jnp.where(chosen, jnp.exp(jnp.where(chosen, logits - top, 0.0)), 0.0)
    g = ex / jnp.sum(ex, axis=1, keepdims=True)
    ET[...] = jnp.transpose(jnp.where(chosen, g, -1.0))
    for r in range(1, 8):
        ecopy(r).start()
    own(1)

    @pl.loop(0, ACC.shape[0])
    def _(i):
        ACC[i] = jnp.zeros((U, U), F32)

    fwd(0)
    for n in range(NWT):
        wtload(n, 0).start()
        wtload(n, 1).start()

    mine = pl.ds(pl.multiple_of(pos_of(0) * EL, EL), EL)
    EX[0:EL] = ET[mine]
    for r in range(1, 8):
        ecopy(r).wait_recv()

    ev = EX[...]
    sel = ev >= 0.0
    before = lax.broadcasted_iota(jnp.int32, (T, T), 0) < lax.broadcasted_iota(jnp.int32, (T, T), 1)
    cnt = _dot(sel.astype(F32).astype(BF), before.astype(F32).astype(BF))
    pos = jnp.where(sel, cnt, -1.0)
    POS[...] = pos

    @pl.loop(0, 8)
    def _(r):
        p = POS[pl.ds(pl.multiple_of(r * EL, EL), EL)]
        slot = lax.broadcasted_iota(jnp.int32, (C, T), 0).astype(F32)
        for e in range(EL):
            HT[r, e * C:(e + 1) * C, :] = jnp.where(jnp.broadcast_to(p[e:e + 1], (C, T)) == slot, 1.0, 0.0).astype(BF)

    ge = jnp.maximum(ev, 0.0)
    post = jnp.transpose(pos).astype(BF)
    gt = jnp.transpose(ge)
    hi = gt.astype(BF)
    rest = gt - hi.astype(F32)
    mid = rest.astype(BF)
    lo = (rest - mid.astype(F32)).astype(BF)

    def weigh(r):
        spread = jnp.where(lax.broadcasted_iota(jnp.int32, (8 * EL, S), 0)
                           == r * EL + lax.broadcasted_iota(jnp.int32, (8 * EL, S), 1) // C, 1.0, 0.0).astype(BF)
        slot = (lax.broadcasted_iota(jnp.int32, (T, S), 1) % C).astype(F32)
        hit = _dot(post, spread) == slot
        for k, part in enumerate((hi, mid, lo)):
            W[k * 8 + r] = jnp.where(hit, _dot(part, spread), 0.0).astype(BF)

    pl.loop(0, 4)(weigh)
    fwd(1)
    own(2)
    own(3)
    pl.loop(4, 8)(weigh)

    def gather(u, s):
        for r in range(8):
            v = _dot(HT[r], X[u * 8 + r])
            XIN[:, r * C:(r + 1) * C, s * U:(s + 1) * U] = v.astype(BF).reshape(EL, C, U)

    def tiles(n):
        for i in range(UE):
            for m in range(2):
                wtload(n + i, m).wait()

    diag(0)
    arrived(0)
    diag(1)
    gather(0, 0)
    arrived(1)

    @pl.loop(0, NQ - 1)
    def _(q):
        u = 2 * q + 2
        gather(u - 1, 1)
        fwd(u)

        @pl.when(u + 2 < NU)
        def _():
            own(u + 2)


        @pl.loop(0, EL // UE)
        def _(g):
            n = q * EL + g * UE
            tiles(n)
            for i in range(UE):
                e, s = g * UE + i, n % NWT + i
                xe = XIN[e]
                for m in range(2):
                    for f in range(NF):
                        ACC[(e * 2 + m) * NF + f] += _dot(xe, WT[s, m, :, f * U:(f + 1) * U])
            @pl.when(g == 1)
            def _():
                diag(u)
                fwd(u + 1)

                @pl.when(u + 3 < NU)
                def _():
                    own(u + 3)

            for i in range(UE):
                for m in range(2):
                    wtload(n + NWT + i, m).start()

        diag(u + 1)
        sent(u - 2)
        sent(u - 1)
        arrived(u)
        gather(u, 0)
        arrived(u + 1)

    gather(NU - 1, 1)

    @pl.loop(0, EL // UE)
    def _(g):
        n = (NQ - 1) * EL + g * UE
        tiles(n)
        for i in range(UE):
            e, s = g * UE + i, n % NWT + i
            xe = XIN[e]
            for f in range(NF):
                a = ACC[e * 2 * NF + f] + _dot(xe, WT[s, 0, :, f * U:(f + 1) * U])
                b = ACC[(e * 2 + 1) * NF + f] + _dot(xe, WT[s, 1, :, f * U:(f + 1) * U])
                X[e * NF + f] = (jax.nn.silu(a) * b).astype(BF)

        @pl.when(n + NWT < NQ * EL)
        def _():
            for i in range(UE):
                for m in range(2):
                    wtload(n + NWT + i, m).start()

        @pl.when((g == 1) | (g == 2))
        def _():
            for i in range(2 * UE):
                w2start(0, (g - 1) * 2 * UE + i)
                w2start(1, (g - 1) * 2 * UE + i)

    for r in (1, 2, 4):
        pl.semaphore_signal(ready, inc=1, device_id=did(r), device_id_type=MESH)

    R1 = 4 * NB
    R2 = R1 + 2 * NB
    YS = R2 + NB
    SS = YS + 8
    TT = SS + 16
    OUT = EL * NF

    def store(b):
        cols = pl.ds(pl.multiple_of(b * 2 * CW, 2 * CW), 2 * CW)
        return pltpu.make_async_copy(X.at[OUT + b], out_hbm.at[:, cols], osem.at[b])

    A = pl.ds(0, CW)
    B = pl.ds(CW, CW)

    def d2d(b, i):
        return pltpu.make_async_remote_copy(
            src_ref=ACC.at[YS + (b % 2) * 4 + i], dst_ref=ACC.at[b * 4 + i],
            send_sem=d2s.at[b, i], recv_sem=d2r.at[b, i], device_id=did(1), device_id_type=MESH)

    def hop1(b, k):
        src, dst, half, to = [(2, 0, A, 4), (3, 1, A, 4), (1, 0, B, 2), (3, 1, B, 2)][k]
        return pltpu.make_async_remote_copy(
            src_ref=ACC.at[SS + (b % 4) * 4 + src, :, half], dst_ref=ACC.at[R1 + b * 2 + dst, :, half],
            send_sem=p1s.at[b, k], recv_sem=p1r.at[b, k], device_id=did(to), device_id_type=MESH)

    def hop2(b, k):
        half, to = [(A, 2), (B, 4)][k]
        return pltpu.make_async_remote_copy(
            src_ref=ACC.at[TT + b % 4, :, half], dst_ref=ACC.at[R2 + b, :, half],
            send_sem=p2s.at[b, k], recv_sem=p2r.at[b, k], device_id=did(to), device_id_type=MESH)

    def combine(r):
        rows = slice(r * C, (r + 1) * C)
        o = XIN[:, rows, 0:2 * CW].reshape(S, 2 * CW)
        return _dot(W[r], o) + _dot(W[8 + r], o) + _dot(W[16 + r], o)

    @pl.loop(0, NB + 3)
    def _(b):
        @pl.when(b < NB)
        def _():
            for e in range(EL):
                for c in w2load(b, e):
                    c.wait()
            for e in range(EL):
                h = jnp.concatenate([X[e * NF + f] for f in range(NF)], axis=1)
                XIN[e, :, 0:2 * CW] = _dot(h, w2tile(b, e)).astype(BF)

            @pl.when(b == 0)
            def _():
                pl.semaphore_wait(ready, 3)

            sb = SS + (b % 4) * 4

            def make(i):
                ACC[YS + (b % 2) * 4 + i] = combine(2 * i + 1)
                d2d(b, i).start()
                ACC[sb + i] = combine(2 * i)

            def total(i, hops):
                d2d(b, i).wait_recv()
                ACC[sb + i] += ACC[b * 4 + i]
                for k in hops:
                    hop1(b, k).start()

            make(3)
            make(2)
            total(3, (1, 3))
            make(1)
            total(2, (0,))
            make(0)
            total(1, (2,))
            total(0, ())
            for i in range(4):
                d2d(b, i).wait_send()

            @pl.when(b == 0)
            def _():
                sent(NU - 2)
                sent(NU - 1)
                for r in range(1, 8):
                    ecopy(r).wait_send()

            @pl.when(b + 2 < NB)
            def _():
                for e in range(EL):
                    w2start(b + 2, e)

        c = b - 1

        @pl.when((c >= 0) & (c < NB))
        def _():
            sc = SS + (c % 4) * 4
            for k, i, half in ((1, 1, slice(0, CW)), (3, 2, slice(CW, 2 * CW))):
                hop1(c, k).wait_recv()
                ACC[TT + c % 4, :, half] = ACC[sc + i, :, half] + ACC[R1 + c * 2 + 1, :, half]
                hop2(c, (k - 1) // 2).start()

        f = b - 3

        @pl.when(f >= 0)
        def _():
            sf = SS + (f % 4) * 4
            for k in range(4):
                hop1(f, k).wait_send()
            hop1(f, 0).wait_recv()
            hop1(f, 2).wait_recv()
            for k, half in ((0, slice(0, CW)), (1, slice(CW, 2 * CW))):
                hop2(f, k).wait_recv()
                X[OUT + f, :, half] = (ACC[sf, :, half] + ACC[R1 + f * 2, :, half] + ACC[R2 + f, :, half]).astype(BF)
                hop2(f, k).wait_send()
            store(f).start()

    @pl.loop(0, NB)
    def _(b):
        store(b).wait()


def solution(mesh):
    tok = P(('data', 'outer', 'expert'), None)
    wsp = P(('outer', 'expert'), None, None)

    def local(x, wr, idx, w1, w3, w2):
        T, D = x.shape
        E = wr.shape[1]
        EL, _, FF = w1.shape
        K = idx.shape[1]
        C = 2 * T * K // E
        S = EL * C
        NU = D // U
        NB = D // (2 * CW)
        NF = FF // U
        any_ = pl.BlockSpec(memory_space=pl.ANY)
        dma = pltpu.SemaphoreType.DMA
        return pl.pallas_call(
            kernel,
            out_shape=jax.ShapeDtypeStruct((T, D), BF),
            in_specs=[any_] * 6,
            out_specs=any_,
            scratch_shapes=[
                pltpu.VMEM((NU * 8, T, U), BF),
                pltpu.VMEM((K, T), jnp.int32),
                pltpu.VMEM((E, T), F32),
                pltpu.VMEM((8 * EL, T), F32),
                pltpu.VMEM((8 * EL, T), F32),
                pltpu.VMEM((8, S, T), BF),
                pltpu.VMEM((24, T, S), BF),
                pltpu.VMEM((EL, 8 * C, 2 * U), BF),
                pltpu.VMEM((EL * 2 * NF, 8 * C, U), F32),
                pltpu.VMEM((NWT, 2, 2 * U, FF), BF),
                dma((2 * NU + 1,)), dma((NWT, 2)), dma((2, EL, 2)),
                dma((8, NU)), dma((8, NU)), dma((8,)), dma((8,)),
                dma((NB, 4)), dma((NB, 4)), dma((NB, 4)), dma((NB, 4)), dma((NB, 2)), dma((NB, 2)), dma((NB,)),
                pltpu.SemaphoreType.REGULAR,
            ],
            compiler_params=pltpu.CompilerParams(collective_id=0, has_side_effects=True, vmem_limit_bytes=67043328),
        )(x, wr, idx.T, w1, w3, w2)

    return jax.shard_map(local, mesh=mesh, in_specs=(tok, P(None, None), tok, wsp, wsp, wsp), out_specs=tok, check_vma=False)
```

```python
import functools

import jax
import jax.numpy as jnp
from jax import lax
from jax.experimental import pallas as pl
from jax.experimental.pallas import tpu as pltpu
from jax.sharding import PartitionSpec as P

MESH = pl.DeviceIdType.MESH
BF = jnp.bfloat16
F32 = jnp.float32
U = 256
CW = 128
NWT = 12
UE = 4


def _dot(a, b):
    return jnp.dot(a, b, preferred_element_type=F32)


def kernel(x_hbm, wr_hbm, idx_hbm, w1_hbm, w3_hbm, w2_hbm, out_hbm,
           X, IDX, ET, EX, POS, HT, W, XIN, ACC, WT,
           xsem, wtsem, w2sem, dsend, drecv, esend, erecv,
           d2s, d2r, p1s, p1r, p2s, p2r, osem, ready):
    T, D = x_hbm.shape
    E = wr_hbm.shape[1]
    EL, _, FF = w1_hbm.shape
    K = idx_hbm.shape[0]
    C = 2 * T * K // E
    S = EL * C
    NU = D // U
    NQ = NU // 2
    NB = D // (2 * CW)
    NF = FF // U

    dd = lax.axis_index("data")
    oy = lax.axis_index("outer")
    jx = lax.axis_index("expert")
    cx = jx // 2
    cc = jx - 2 * cx
    nx = lax.axis_size("expert")

    def dev(r):
        ry, rx, rc = r // 4, (r // 2) % 2, r % 2
        y = 1 - oy if ry else oy
        x = 1 - cx if rx else cx
        c = 1 - cc if rc else cc
        return y, x * 2 + c

    def did(r):
        y, j = dev(r)
        return (dd, y, j)

    def pos_of(r):
        y, j = dev(r)
        return y * nx + j

    def xload(u):
        return pltpu.make_async_copy(x_hbm.at[:, pl.ds(u * U, U)], X.at[u * 8], xsem.at[u])

    def wrload(u):
        return pltpu.make_async_copy(wr_hbm.at[pl.ds(u * U, U)], XIN.at[u, :, 0:E], xsem.at[NU + u])

    idxload = pltpu.make_async_copy(idx_hbm, IDX, xsem.at[2 * NU])

    def wtload(n, m):
        q, e, s = n // EL, n % EL, n % NWT
        src = w1_hbm if m == 0 else w3_hbm
        rows = pl.ds(pl.multiple_of(q * 2 * U, 2 * U), 2 * U)
        return pltpu.make_async_copy(src.at[e, rows, :], WT.at[s, m], wtsem.at[s, m])

    R = 2 * U

    def w2place(b, e):
        p = b % 2
        s, m = NWT - EL // 2 + e // 2, e % 2
        return ((s, m, slice(None), pl.ds(pl.multiple_of(p * 4 * CW, 4 * CW), 2 * CW)),
                (s, m, pl.ds(pl.multiple_of(p * (FF - R), FF - R), FF - R), slice(2 * CW, 4 * CW)))

    def w2load(b, e):
        cols = pl.ds(pl.multiple_of(b * 2 * CW, 2 * CW), 2 * CW)
        top, low = w2place(b, e)
        return (pltpu.make_async_copy(w2_hbm.at[e, 0:R, cols], WT.at[top], w2sem.at[b % 2, e, 0]),
                pltpu.make_async_copy(w2_hbm.at[e, R:FF, cols], WT.at[low], w2sem.at[b % 2, e, 1]))

    def w2start(b, e):
        for c in w2load(b, e):
            c.start()

    def w2tile(b, e):
        top, low = w2place(b, e)
        return jnp.concatenate([WT[top], WT[low]], axis=0)

    H = T // 2

    def blk(u, r, half=None):
        b = u * 8 + r
        if half is None:
            return X.at[b]
        return X.at[b, pl.ds(half * H, H)]

    def disp(k, u):
        src, dst, to = [
            (blk(u, 0), blk(u, 2), 2), (blk(u, 0), blk(u, 4), 4), (blk(u, 0), blk(u, 1), 1),
            (blk(u, 2, 0), blk(u, 6, 0), 4), (blk(u, 4, 1), blk(u, 6, 1), 2),
            (blk(u, 2), blk(u, 3), 1), (blk(u, 4), blk(u, 5), 1), (blk(u, 6), blk(u, 7), 1),
        ][k]
        return pltpu.make_async_remote_copy(src_ref=src, dst_ref=dst, send_sem=dsend.at[k, u], recv_sem=drecv.at[k, u],
                                            device_id=did(to), device_id_type=MESH)

    def own(u):
        for k in (0, 1, 2):
            disp(k, u).start()

    def fwd(u):
        disp(0, u).wait_recv()
        disp(1, u).wait_recv()
        for k in (3, 4, 5, 6):
            disp(k, u).start()

    def diag(u):
        disp(3, u).wait_recv()
        disp(4, u).wait_recv()
        disp(7, u).start()

    def arrived(u):
        for k in (2, 5, 6, 7):
            disp(k, u).wait_recv()

    def sent(u):
        for k in range(8):
            disp(k, u).wait_send()

    def ecopy(r):
        rows = pl.ds(pl.multiple_of(pos_of(r) * EL, EL), EL)
        return pltpu.make_async_remote_copy(src_ref=ET.at[rows], dst_ref=EX.at[pl.ds(r * EL, EL)],
                                            send_sem=esend.at[r], recv_sem=erecv.at[r],
                                            device_id=did(r), device_id_type=MESH)

    for u in range(NU):
        xload(u).start()
    for u in range(NU):
        wrload(u).start()
    idxload.start()

    barrier = pltpu.get_barrier_semaphore()
    for r in range(1, 8):
        pl.semaphore_signal(barrier, inc=1, device_id=did(r), device_id_type=MESH)
    xload(0).wait()
    pl.semaphore_wait(barrier, 7)
    own(0)

    for u in range(1, NU):
        xload(u).wait()
    for u in range(NU):
        wrload(u).wait()
    idxload.wait()
    logits = _dot(X[0], XIN[0, :, 0:E])
    for u in range(1, NU):
        logits = logits + _dot(X[u * 8], XIN[u, :, 0:E])
    lane = lax.broadcasted_iota(jnp.int32, (T, E), 1)
    ids = jnp.transpose(IDX[...].astype(F32)).astype(jnp.int32)
    chosen = lane == ids[:, 0:1]
    for j in range(1, K):
        chosen = chosen | (lane == ids[:, j:j + 1])
    top = jnp.max(jnp.where(chosen, logits, -jnp.inf), axis=1, keepdims=True)
    ex = jnp.where(chosen, jnp.exp(jnp.where(chosen, logits - top, 0.0)), 0.0)
    g = ex / jnp.sum(ex, axis=1, keepdims=True)
    ET[...] = jnp.transpose(jnp.where(chosen, g, -1.0))
    for r in range(1, 8):
        ecopy(r).start()
    own(1)

    @pl.loop(0, ACC.shape[0])
    def _(i):
        ACC[i] = jnp.zeros((U, U), F32)

    fwd(0)
    for n in range(NWT):
        wtload(n, 0).start()
        wtload(n, 1).start()

    mine = pl.ds(pl.multiple_of(pos_of(0) * EL, EL), EL)
    EX[0:EL] = ET[mine]
    for r in range(1, 8):
        ecopy(r).wait_recv()

    ev = EX[...]
    sel = ev >= 0.0
    before = lax.broadcasted_iota(jnp.int32, (T, T), 0) < lax.broadcasted_iota(jnp.int32, (T, T), 1)
    cnt = _dot(sel.astype(F32).astype(BF), before.astype(F32).astype(BF))
    pos = jnp.where(sel, cnt, -1.0)
    POS[...] = pos

    @pl.loop(0, 8)
    def _(r):
        p = POS[pl.ds(pl.multiple_of(r * EL, EL), EL)]
        slot = lax.broadcasted_iota(jnp.int32, (C, T), 0).astype(F32)
        for e in range(EL):
            HT[r, e * C:(e + 1) * C, :] = jnp.where(jnp.broadcast_to(p[e:e + 1], (C, T)) == slot, 1.0, 0.0).astype(BF)

    ge = jnp.maximum(ev, 0.0)
    post = jnp.transpose(pos).astype(BF)
    gt = jnp.transpose(ge)
    hi = gt.astype(BF)
    rest = gt - hi.astype(F32)
    mid = rest.astype(BF)
    lo = (rest - mid.astype(F32)).astype(BF)

    def weigh(r):
        spread = jnp.where(lax.broadcasted_iota(jnp.int32, (8 * EL, S), 0)
                           == r * EL + lax.broadcasted_iota(jnp.int32, (8 * EL, S), 1) // C, 1.0, 0.0).astype(BF)
        slot = (lax.broadcasted_iota(jnp.int32, (T, S), 1) % C).astype(F32)
        hit = _dot(post, spread) == slot
        for k, part in enumerate((hi, mid, lo)):
            W[k * 8 + r] = jnp.where(hit, _dot(part, spread), 0.0).astype(BF)

    pl.loop(0, 4)(weigh)
    fwd(1)
    own(2)
    own(3)
    pl.loop(4, 8)(weigh)

    def gather(u, s):
        for r in range(8):
            v = _dot(HT[r], X[u * 8 + r])
            XIN[:, r * C:(r + 1) * C, s * U:(s + 1) * U] = v.astype(BF).reshape(EL, C, U)

    def tiles(n):
        for i in range(UE):
            for m in range(2):
                wtload(n + i, m).wait()

    diag(0)
    arrived(0)
    diag(1)
    gather(0, 0)
    arrived(1)

    @pl.loop(0, NQ - 1)
    def _(q):
        u = 2 * q + 2
        gather(u - 1, 1)
        fwd(u)

        @pl.when(u + 2 < NU)
        def _():
            own(u + 2)


        for g in range(EL // UE):
            n = q * EL + g * UE
            tiles(n)
            for i in range(UE):
                e, s = g * UE + i, n % NWT + i
                xe = XIN[e]
                for m in range(2):
                    for f in range(NF):
                        ACC[(e * 2 + m) * NF + f] += _dot(xe, WT[s, m, :, f * U:(f + 1) * U])
            if g == 1:
                diag(u)
                fwd(u + 1)

                @pl.when(u + 3 < NU)
                def _():
                    own(u + 3)

            for i in range(UE):
                for m in range(2):
                    wtload(n + NWT + i, m).start()

        diag(u + 1)
        sent(u - 2)
        sent(u - 1)
        arrived(u)
        gather(u, 0)
        arrived(u + 1)

    gather(NU - 1, 1)

    for g in range(EL // UE):
        n = (NQ - 1) * EL + g * UE
        tiles(n)
        for i in range(UE):
            e, s = g * UE + i, n % NWT + i
            xe = XIN[e]
            for f in range(NF):
                a = ACC[e * 2 * NF + f] + _dot(xe, WT[s, 0, :, f * U:(f + 1) * U])
                b = ACC[(e * 2 + 1) * NF + f] + _dot(xe, WT[s, 1, :, f * U:(f + 1) * U])
                X[e * NF + f] = (jax.nn.silu(a) * b).astype(BF)
        if n + NWT < NQ * EL:
            for i in range(UE):
                for m in range(2):
                    wtload(n + NWT + i, m).start()
        elif g == 1 or g == 2:
            for i in range(2 * UE):
                w2start(0, (g - 1) * 2 * UE + i)
                w2start(1, (g - 1) * 2 * UE + i)

    for r in (1, 2, 4):
        pl.semaphore_signal(ready, inc=1, device_id=did(r), device_id_type=MESH)

    R1 = 4 * NB
    R2 = R1 + 2 * NB
    YS = R2 + NB
    SS = YS + 8
    TT = SS + 16
    OUT = EL * NF

    def store(b):
        cols = pl.ds(pl.multiple_of(b * 2 * CW, 2 * CW), 2 * CW)
        return pltpu.make_async_copy(X.at[OUT + b], out_hbm.at[:, cols], osem.at[b])

    A = pl.ds(0, CW)
    B = pl.ds(CW, CW)

    def d2d(b, i):
        return pltpu.make_async_remote_copy(
            src_ref=ACC.at[YS + (b % 2) * 4 + i], dst_ref=ACC.at[b * 4 + i],
            send_sem=d2s.at[b, i], recv_sem=d2r.at[b, i], device_id=did(1), device_id_type=MESH)

    def hop1(b, k):
        src, dst, half, to = [(2, 0, A, 4), (3, 1, A, 4), (1, 0, B, 2), (3, 1, B, 2)][k]
        return pltpu.make_async_remote_copy(
            src_ref=ACC.at[SS + (b % 4) * 4 + src, :, half], dst_ref=ACC.at[R1 + b * 2 + dst, :, half],
            send_sem=p1s.at[b, k], recv_sem=p1r.at[b, k], device_id=did(to), device_id_type=MESH)

    def hop2(b, k):
        half, to = [(A, 2), (B, 4)][k]
        return pltpu.make_async_remote_copy(
            src_ref=ACC.at[TT + b % 4, :, half], dst_ref=ACC.at[R2 + b, :, half],
            send_sem=p2s.at[b, k], recv_sem=p2r.at[b, k], device_id=did(to), device_id_type=MESH)

    def combine(r):
        rows = slice(r * C, (r + 1) * C)
        o = XIN[:, rows, 0:2 * CW].reshape(S, 2 * CW)
        return _dot(W[r], o) + _dot(W[8 + r], o) + _dot(W[16 + r], o)

    @pl.loop(0, NB + 3)
    def _(b):
        @pl.when(b < NB)
        def _():
            for e in range(EL):
                for c in w2load(b, e):
                    c.wait()
            for e in range(EL):
                h = jnp.concatenate([X[e * NF + f] for f in range(NF)], axis=1)
                XIN[e, :, 0:2 * CW] = _dot(h, w2tile(b, e)).astype(BF)

            @pl.when(b == 0)
            def _():
                pl.semaphore_wait(ready, 3)

            sb = SS + (b % 4) * 4

            def make(i):
                ACC[YS + (b % 2) * 4 + i] = combine(2 * i + 1)
                d2d(b, i).start()
                ACC[sb + i] = combine(2 * i)

            def total(i, hops):
                d2d(b, i).wait_recv()
                ACC[sb + i] += ACC[b * 4 + i]
                for k in hops:
                    hop1(b, k).start()

            make(3)
            make(2)
            total(3, (1, 3))
            make(1)
            total(2, (0,))
            make(0)
            total(1, (2,))
            total(0, ())
            for i in range(4):
                d2d(b, i).wait_send()

            @pl.when(b == 0)
            def _():
                sent(NU - 2)
                sent(NU - 1)
                for r in range(1, 8):
                    ecopy(r).wait_send()

            @pl.when(b + 2 < NB)
            def _():
                for e in range(EL):
                    w2start(b + 2, e)

        c = b - 1

        @pl.when((c >= 0) & (c < NB))
        def _():
            sc = SS + (c % 4) * 4
            for k, i, half in ((1, 1, slice(0, CW)), (3, 2, slice(CW, 2 * CW))):
                hop1(c, k).wait_recv()
                ACC[TT + c % 4, :, half] = ACC[sc + i, :, half] + ACC[R1 + c * 2 + 1, :, half]
                hop2(c, (k - 1) // 2).start()

        f = b - 3

        @pl.when(f >= 0)
        def _():
            sf = SS + (f % 4) * 4
            for k in range(4):
                hop1(f, k).wait_send()
            hop1(f, 0).wait_recv()
            hop1(f, 2).wait_recv()
            for k, half in ((0, slice(0, CW)), (1, slice(CW, 2 * CW))):
                hop2(f, k).wait_recv()
                X[OUT + f, :, half] = (ACC[sf, :, half] + ACC[R1 + f * 2, :, half] + ACC[R2 + f, :, half]).astype(BF)
                hop2(f, k).wait_send()
            store(f).start()

    @pl.loop(0, NB)
    def _(b):
        store(b).wait()


def solution(mesh):
    tok = P(('data', 'outer', 'expert'), None)
    wsp = P(('outer', 'expert'), None, None)

    def local(x, wr, idx, w1, w3, w2):
        T, D = x.shape
        E = wr.shape[1]
        EL, _, FF = w1.shape
        K = idx.shape[1]
        C = 2 * T * K // E
        S = EL * C
        NU = D // U
        NB = D // (2 * CW)
        NF = FF // U
        any_ = pl.BlockSpec(memory_space=pl.ANY)
        dma = pltpu.SemaphoreType.DMA
        return pl.pallas_call(
            kernel,
            out_shape=jax.ShapeDtypeStruct((T, D), BF),
            in_specs=[any_] * 6,
            out_specs=any_,
            scratch_shapes=[
                pltpu.VMEM((NU * 8, T, U), BF),
                pltpu.VMEM((K, T), jnp.int32),
                pltpu.VMEM((E, T), F32),
                pltpu.VMEM((8 * EL, T), F32),
                pltpu.VMEM((8 * EL, T), F32),
                pltpu.VMEM((8, S, T), BF),
                pltpu.VMEM((24, T, S), BF),
                pltpu.VMEM((EL, 8 * C, 2 * U), BF),
                pltpu.VMEM((EL * 2 * NF, 8 * C, U), F32),
                pltpu.VMEM((NWT, 2, 2 * U, FF), BF),
                dma((2 * NU + 1,)), dma((NWT, 2)), dma((2, EL, 2)),
                dma((8, NU)), dma((8, NU)), dma((8,)), dma((8,)),
                dma((NB, 4)), dma((NB, 4)), dma((NB, 4)), dma((NB, 4)), dma((NB, 2)), dma((NB, 2)), dma((NB,)),
                pltpu.SemaphoreType.REGULAR,
            ],
            compiler_params=pltpu.CompilerParams(collective_id=0, has_side_effects=True, vmem_limit_bytes=67043328),
        )(x, wr, idx.T, w1, w3, w2)

    return jax.shard_map(local, mesh=mesh, in_specs=(tok, P(None, None), tok, wsp, wsp, wsp), out_specs=tok, check_vma=False)
```
